128 devices in a mesh: expert: 16 (over y, x), mp: 8 (over z, core).
Axes of the slice: x: 4, y: 4, z: 4, core: 2. Of those that a mesh axis runs over, the one named last changes fastest.
Arguments:
- tokens: bfloat16 [2048, 7168], P('expert', 'mp'), may hold values from -0.625 to 0.625
- cotangent: bfloat16 [2048, 8, 2048], P('expert', None, 'mp'), may hold values from -3 to 3
- weights: bfloat16 [32, 7168, 2048], P('expert', 'mp'), may hold values from -0.0625 to 0.0625
- steps: float32 [32, 2048], P('expert', 'mp'), may hold values from 0.002 to 0.02
- expert_ids: int32 [2048, 8], P('expert'), may hold values from 0 to 31, all different within a row; in each aligned block of 128 rows (0 to 127, 128 to 255, ...) at most 64 rows name the same one
Outputs:
- token_grads: bfloat16 [2048, 7168], P('expert', 'mp')
- weight_grads: bfloat16 [32, 7168, 2048], P('expert', 'mp')
- step_grads: float32 [32, 2048], P('expert', 'mp')
The draws below stay inside these ranges and needn't reach their ends.
Inputs may be any that keep to these rules, and one draw needn't show every extreme that they name: `expert_ids`: each row names 8 different experts; among the 128 rows of one index of the expert axis, no expert is named by more than 64 rows, a bound that some block reaches of them.
All inputs are finite; a program needn't handle non-finite values.
Results may differ from the reference program's by a relative error of at most 0.0058.
Values may be sent and summed in bfloat16 or wider, within the bound.
A program may use at most 128 MiB of HBM per device.

```python
import math
import jax
import jax.numpy as jnp
import numpy as np
from jax import lax

D = 7168
FF = 2048
TOP = 8
TOK_DEV = 128
EXPERTS = 32
CAP = 64
TOKENS = 2048
N_EXPERT = 16


def level_of(stream_key, shape, shards, smallest, largest):
    level, own = 1.0, jax.random.fold_in(stream_key, 6)
    for dim, shards_of in shards:
        draws = jnp.exp(jax.random.uniform(jax.random.fold_in(own, dim), (shards_of,), jnp.float32, smallest / len(shards), largest / len(shards)))
        level = level * jnp.repeat(draws, shape[dim] // shards_of).reshape([-1 if axis == dim else 1 for axis in range(len(shape))])
    return level


def assign_block(rng, own, number, rows, number_of, top, bound, skew):
    sequence = jax.random.permutation(rng, number_of)
    heavy_load, common = shares(number_of, rows * top, bound, skew, True), shares(number_of, rows * top, bound, skew, False)
    places = jnp.arange(number_of)

    def named(sizes, rotation):
        used = int((sizes > 0).sum())
        fixed = max(1, used // 4)
        moved = fixed + (places - fixed + rotation * (used - fixed)) % max(1, number_of - fixed)
        return jnp.zeros((number_of,), jnp.int32).at[sequence[jnp.where(places < fixed, places, moved)]].set(jnp.asarray(sizes, jnp.int32))

    sizes = jnp.where(number % 4 == 0, named(heavy_load, number // 4), named(common, number - number // 4 - 1))
    mixed = jax.random.permutation(jax.random.fold_in(own, 3), number_of)
    donor, taker = mixed[0:number_of // 2 * 2:2], mixed[1:number_of // 2 * 2:2]
    room = jnp.minimum(sizes[donor] - 1, bound - sizes[taker]) // 2
    room = jnp.where((donor == sequence[0]) | (taker == sequence[0]) | (sizes[taker] == 0), 0, jnp.maximum(room, 0))
    moved = jax.random.randint(jax.random.fold_in(own, 4), (number_of // 2,), 0, 1 << 20) % (room + 1)
    sizes = sizes.at[donor].add(-moved).at[taker].add(moved)
    items = jnp.searchsorted(jnp.cumsum(sizes), jnp.arange(rows * top), side="right").astype(jnp.int32)
    table = items.reshape(top, rows).T
    table = table[jax.random.permutation(jax.random.fold_in(own, 1), rows)]
    rotation = jax.random.randint(jax.random.fold_in(own, 2), (rows, 1), 0, top)
    return jnp.take_along_axis(table, (jnp.arange(top)[None, :] + rotation) % top, axis=1)


def shares(number_of, total, bound, slope, full):
    weights = [(1 << 20) // math.isqrt(grade ** slope) + 1 for grade in range(1, number_of + 1)]
    largest = bound if full else min(bound, max(-(-total // number_of), total * weights[0] // sum(weights)))
    least = 1 if total - largest >= number_of - 1 else 0
    given, rest = [largest] + [least] * (number_of - 1), total - largest - least * (number_of - 1)
    while rest > 0:
        movable = [i for i in range(1, number_of) if given[i] < largest] or [i for i in range(1, number_of) if given[i] < bound]
        whole, left = sum([weights[i] for i in movable]), rest
        for i in movable:
            more = min(bound - given[i], max(1, left * weights[i] // whole), rest)
            given[i] = given[i] + more
            rest = rest - more
    return np.array(given)


def normal_values(own_key, extent, scale, reach, shards=(), kind=jnp.bfloat16):
    result = scale * jax.random.normal(own_key, extent, jnp.float32)
    if shards:
        result = result * level_of(own_key, extent, shards, -0.22, 0.18)
    return jnp.clip(result, -reach, reach).astype(kind)


def setup_inputs(seed: int = 0) -> dict:
    splits = jax.random.split(jax.random.key(seed), 6)
    tokens = normal_values(splits[0], (TOKENS, D), 0.1, 0.625, ((0, 16), (1, 8)))
    cotangent = normal_values(splits[1], (TOKENS, TOP, FF), 0.5, 3.0, ((0, 16), (2, 8)))
    weights = normal_values(splits[2], (EXPERTS, D, FF), D ** -0.5, 0.0625, ((0, 16), (1, 8)))
    steps = jnp.clip(jnp.exp(math.log(0.02) - 2.30258502 * jax.random.uniform(splits[3], (EXPERTS, FF), jnp.float32) ** level_of(splits[3], (EXPERTS, FF), ((0, 16), (1, 8)), -0.2, 0.2)), 0.002, 0.02)
    expert_ids_keys = jax.random.split(jax.random.fold_in(splits[4], 1), TOKENS // TOK_DEV)
    expert_ids_turns = jax.random.permutation(jax.random.fold_in(splits[4], 3), TOKENS // TOK_DEV)
    expert_ids = jax.vmap(lambda own, number: assign_block(jax.random.fold_in(splits[4], 2), own, number, TOK_DEV, EXPERTS, TOP, CAP, 2))(expert_ids_keys, expert_ids_turns).reshape((TOKENS, TOP))
    return dict(tokens=tokens, cotangent=cotangent, weights=weights, steps=steps, expert_ids=expert_ids)


qmax = 7.0
wiggle = 0.9
two_pi = 6.283185307179586

def quantize(weight_f, step_f):
    scaled = weight_f / step_f
    squash = jnp.tanh(scaled / qmax)
    clipped = qmax * squash
    angles = two_pi * clipped
    stair = clipped - wiggle * jnp.sin(angles) / two_pi
    slopes = (1.0 - wiggle * jnp.cos(angles)) * (1.0 - squash * squash)
    return (step_f * stair, slopes, stair - scaled * slopes)

def slot_table(routes_flat, experts, capacity):
    one_hot = (routes_flat[:, None] == jnp.arange(experts, dtype=jnp.int32)[None, :]).astype(jnp.int32)
    before = jnp.cumsum(one_hot, axis=0) - one_hot
    position = lax.optimization_barrier(jnp.sum(before * one_hot, axis=1))
    slot_of = (routes_flat * capacity + position).astype(jnp.int32)
    route_count = routes_flat.shape[0]
    source_of = jnp.full((experts * capacity,), route_count, jnp.int32)
    source_of = source_of.at[slot_of].set(jnp.arange(route_count, dtype=jnp.int32))
    return (slot_of, source_of)

def reference(tokens, cotangent, weights, steps, expert_ids):
    blocks = expert_ids.reshape(N_EXPERT, TOK_DEV * TOP)
    sources = jax.vmap(lambda block_rows: slot_table(block_rows, EXPERTS, CAP)[1])(blocks)
    offsets = (jnp.arange(N_EXPERT, dtype=jnp.int32) * (TOK_DEV * TOP))[:, None]
    sentinel = TOKENS * TOP
    global_src = jnp.where(sources < TOK_DEV * TOP, sources + offsets, sentinel).astype(jnp.int32)
    per_expert = global_src.reshape(N_EXPERT, EXPERTS, CAP).transpose(1, 0, 2).reshape(EXPERTS, N_EXPERT * CAP)
    padded_x = jnp.concatenate([tokens, jnp.zeros((1, D), tokens.dtype)], axis=0)
    padded_g = jnp.concatenate([cotangent.reshape(TOKENS * TOP, FF), jnp.zeros((1, FF), cotangent.dtype)], axis=0)
    grad_scale = 1.0 / math.sqrt(D * qmax)

    def one_expert(running, inputs):
        weight_e, step_e, route_e = inputs
        token_e = (route_e // TOP).astype(jnp.int32)
        rows_x = padded_x[token_e]
        rows_g = padded_g[route_e]
        levels, slopes, step_slopes = quantize(weight_e.astype(jnp.float32), step_e[None, :])
        quantized = levels.astype(jnp.bfloat16)
        raw = jnp.dot(rows_x.T, rows_g, preferred_element_type=jnp.float32)
        out_weight = (raw * slopes).astype(jnp.bfloat16)
        out_step = grad_scale * lax.optimization_barrier(jnp.sum(raw * step_slopes, axis=0))
        back = jnp.dot(rows_g, quantized.T, preferred_element_type=jnp.float32).astype(jnp.bfloat16)
        running = running.at[token_e].add(back.astype(jnp.float32))
        return (running, (out_weight, out_step))
    start_sum = jnp.zeros((TOKENS + 1, D), jnp.float32)
    summed, (weight_grads, step_grads) = lax.scan(one_expert, start_sum, (weights, steps, per_expert))
    return (summed[:TOKENS].astype(jnp.bfloat16), weight_grads, step_grads)
```

```python
import functools
import math

import jax
import jax.numpy as jnp
from jax import lax
from jax.experimental import pallas as pl
from jax.experimental.pallas import tpu as pltpu
from jax.sharding import PartitionSpec as P

qmax = 7.0
wiggle = 0.9
two_pi = 6.283185307179586
F32 = jnp.float32
BF16 = jnp.bfloat16

SIN = (3.141592640130707, -5.167710083507862, 2.550077523214134, -0.5982912856178576, 0.0776576603009221)
COS = (0.9999999532476082, -4.93479283061961, 4.058411352862034, -1.3318765680776314, 0.2196896110917421)


def poly(z, coefs):
    total = coefs[-1] * z + coefs[-2]
    for coef in coefs[-3::-1]:
        total = total * z + coef
    return total


def quantize(w, step, inv7):
    t = w * inv7
    u = jnp.tanh(t)
    c = qmax * u
    r = c - jnp.floor(c + 0.5)
    z = r * r
    sine = r * poly(z, SIN)
    cosine = poly(z, COS)
    stair = c - (2.0 * wiggle / two_pi) * (sine * cosine)
    slopes = ((1.0 - wiggle) + (2.0 * wiggle) * (sine * sine)) * (1.0 - u * u)
    return step * stair, slopes, stair - (qmax * t) * slopes


def dot(a, b, ca, cb):
    return lax.dot_general(a, b, (((ca,), (cb,)), ((), ())), preferred_element_type=F32)


def upper(n):
    rows = lax.broadcasted_iota(jnp.int32, (n, n), 0)
    cols = lax.broadcasted_iota(jnp.int32, (n, n), 1)
    return jnp.where(rows < cols, 1.0, 0.0).astype(BF16)


def pack_kernel(cap, experts, ids_ref, cot_ref, out_ref):
    chunks = ids_ref.shape[0]
    ahead = upper(128)
    expert = lax.broadcasted_iota(jnp.int32, (experts, 128), 0)
    base = expert.astype(F32) * float(cap)
    seen = jnp.zeros((experts, 1), F32)
    slots = []
    for c in range(chunks):
        hot = jnp.where(expert == ids_ref[c : c + 1, :], 1.0, 0.0)
        place = dot(hot.astype(BF16), ahead, 1, 0) + seen + base
        slots.append(jnp.sum(hot * place, axis=0, keepdims=True))
        seen = seen + jnp.sum(hot, axis=1, keepdims=True)
    slot_row = jnp.concatenate(slots, axis=1).astype(jnp.int32)
    rows = lax.broadcasted_iota(jnp.int32, (128, chunks * 128), 0)
    for j in range(experts * cap // 128):
        pick = jnp.where(rows + 128 * j == slot_row, 1.0, 0.0).astype(BF16)
        out_ref[pl.ds(128 * j, 128), :] = dot(pick, cot_ref[...], 1, 0).astype(BF16)


def pack(ids_rows, cot, cap, experts):
    return pl.pallas_call(
        functools.partial(pack_kernel, cap, experts),
        out_shape=jax.ShapeDtypeStruct((experts * cap, cot.shape[1]), BF16),
        name="pack",
    )(ids_rows, cot)


def quant_kernel(w_ref, s_ref, q_ref, a_ref, b_ref):
    rows, width = w_ref.shape[1:]
    step_rows, step_cols = 16, 512
    for col in range(0, width, step_cols):
        cols = pl.ds(col, step_cols)
        s = s_ref[0, :, cols]
        inv7 = 1.0 / (qmax * s)

        def body(k, carry):
            at = pl.ds(pl.multiple_of(k * step_rows, step_rows), step_rows)
            w = w_ref[0, at, cols].astype(F32)
            q, slopes, step_slopes = quantize(w, s, inv7)
            q_ref[0, at, cols] = q.astype(BF16)
            a_ref[0, at, cols] = slopes.astype(BF16)
            b_ref[0, at, cols] = step_slopes.astype(BF16)
            return carry

        lax.fori_loop(0, rows // step_rows, body, 0, unroll=2)


def quant(weights, steps):
    e, d, f = weights.shape
    tile = 128
    block = pl.BlockSpec((1, tile, f), lambda i, j: (i, j, 0))
    return pl.pallas_call(
        quant_kernel,
        grid=(e, d // tile),
        in_specs=[block, pl.BlockSpec((1, 1, f), lambda i, j: (i, 0, 0))],
        out_specs=[block] * 3,
        out_shape=[jax.ShapeDtypeStruct((e, d, f), BF16)] * 3,
        cost_estimate=pl.CostEstimate(flops=50 * e * d * f, bytes_accessed=8 * e * d * f, transcendentals=e * d * f),
        name="quant",
    )(weights, steps)


def selection(ids_ref, first, local, cap):
    groups, _, toks = ids_ref.shape
    ahead = upper(toks)
    picks = []
    for e in range(local):
        named = [jnp.max(jnp.where(ids_ref[i] == first + e, 1.0, 0.0), axis=0, keepdims=True) for i in range(groups)]
        named = jnp.concatenate(named, axis=0)
        place = dot(named.astype(BF16), ahead, 1, 0)
        picks.append(jnp.where(named > 0.0, place, -1.0).astype(jnp.int32))
    return picks


def pick_of(places, i, cap):
    slot = lax.broadcasted_iota(jnp.int32, (cap, places.shape[1]), 0)
    return jnp.where(slot == places[i : i + 1, :], 1.0, 0.0).astype(BF16)


def back_kernel(cap, ids_ref, g_ref, q_ref, out_ref, sums, backs):
    e = pl.program_id(0)
    local = pl.num_programs(0)
    groups = ids_ref.shape[0]
    g = g_ref[...].reshape(groups * cap, g_ref.shape[-1])
    backs[...] = dot(g, q_ref[0], 1, 1).astype(BF16)
    places = selection(ids_ref, lax.axis_index("expert") * local + e, 1, cap)[0]
    for i in range(groups):
        part = dot(pick_of(places, i, cap), backs[pl.ds(i * cap, cap), :], 0, 0)

        @pl.when(e == 0)
        def _():
            sums[i] = part

        @pl.when(e > 0)
        def _():
            out_ref[i] = (sums[i] + part).astype(BF16)


def back(ids, g, q):
    groups, local, cap, f = g.shape
    d = q.shape[1]
    toks = ids.shape[2]
    return pl.pallas_call(
        functools.partial(back_kernel, cap),
        grid=(local,),
        in_specs=[
            pl.BlockSpec(ids.shape, lambda e: (0, 0, 0)),
            pl.BlockSpec((groups, 1, cap, f), lambda e: (0, e, 0, 0)),
            pl.BlockSpec((1, d, f), lambda e: (e, 0, 0)),
        ],
        out_specs=pl.BlockSpec((groups, toks, d), lambda e: (0, 0, 0)),
        out_shape=jax.ShapeDtypeStruct((groups, toks, d), BF16),
        scratch_shapes=[pltpu.VMEM((groups, toks, d), F32), pltpu.VMEM((groups * cap, d), BF16)],
        cost_estimate=pl.CostEstimate(flops=2 * groups * local * cap * f * d, bytes_accessed=20 << 20, transcendentals=0),
        name="back",
    )(ids, g, q)


def raw_kernel(cap, ids_ref, x_ref, g_ref, a_ref, b_ref, w_ref, s_ref, picked):
    e = pl.program_id(0)
    local = pl.num_programs(0)
    groups = ids_ref.shape[0]

    @pl.when(pl.program_id(1) == 0)
    def _():
        places = selection(ids_ref, lax.axis_index("expert") * local + e, 1, cap)[0]
        for i in range(groups):
            part = dot(pick_of(places, i, cap), x_ref[i], 1, 0).astype(BF16)
            picked[:, pl.ds(i * cap, cap)] = part.T

    g = g_ref[...].reshape(groups * cap, g_ref.shape[-1])
    raw = dot(picked[...], g, 1, 0)
    w_ref[0] = (raw * a_ref[0].astype(F32)).astype(BF16)
    s_ref[0] = jnp.sum(raw * b_ref[0].astype(F32), axis=0, keepdims=True)


def raw_grads(ids, x, g, slopes, step_slopes):
    groups, local, cap, f = g.shape
    d = slopes.shape[1]
    tile = 256
    block = pl.BlockSpec((1, d, tile), lambda e, j: (e, 0, j))
    return pl.pallas_call(
        functools.partial(raw_kernel, cap),
        grid=(local, f // tile),
        in_specs=[
            pl.BlockSpec(ids.shape, lambda e, j: (0, 0, 0)),
            pl.BlockSpec(x.shape, lambda e, j: (0, 0, 0)),
            pl.BlockSpec((groups, 1, cap, tile), lambda e, j: (0, e, 0, j)),
            block,
            block,
        ],
        out_specs=[block, pl.BlockSpec((1, 1, tile), lambda e, j: (e, 0, j))],
        out_shape=[jax.ShapeDtypeStruct((local, d, f), BF16), jax.ShapeDtypeStruct((local, 1, f), F32)],
        scratch_shapes=[pltpu.VMEM((d, groups * cap), BF16)],
        cost_estimate=pl.CostEstimate(flops=2 * groups * local * cap * f * d, bytes_accessed=40 << 20, transcendentals=0),
        name="raw",
    )(ids, x, g, slopes, step_slopes)


def per_device(tokens, cotangent, weights, steps, expert_ids):
    groups = lax.axis_size("expert")
    parts = lax.axis_size("mp")
    local = weights.shape[0]
    experts = groups * local
    toks, top_k = expert_ids.shape
    cap = toks // 2
    width = tokens.shape[1]
    part_f = cotangent.shape[2]
    packed = pack(expert_ids.reshape(-1, 128), cotangent.reshape(toks * top_k, part_f), cap, experts)
    ids = lax.all_gather(expert_ids.T, "expert", axis=0)
    x = lax.all_gather(tokens, "expert", axis=0)
    full_steps = lax.all_gather(steps, "mp", axis=1, tiled=True).reshape(local, 1, -1)
    g_part = lax.all_to_all(packed.reshape(groups, local, cap, part_f), "expert", split_axis=0, concat_axis=0, tiled=True)
    g = lax.all_gather(g_part, "mp", axis=3, tiled=True)
    q, slopes, step_slopes = quant(weights, full_steps)
    backs = back(ids, g, q)
    returned = lax.all_to_all(backs, "expert", split_axis=0, concat_axis=0, tiled=True)
    weight_out, partial_steps = raw_grads(ids, x, g, slopes, step_slopes)
    token_out = returned.astype(F32).sum(axis=0).astype(BF16)
    shares = partial_steps.reshape(local, parts, part_f).transpose(1, 0, 2)
    shares = lax.all_to_all(shares, "mp", split_axis=0, concat_axis=0, tiled=True)
    step_out = shares.sum(axis=0) * (1.0 / math.sqrt(width * parts * qmax))
    return (token_out, weight_out, step_out)


def solution(mesh):
    return jax.shard_map(
        per_device,
        mesh=mesh,
        in_specs=(
            P("expert", "mp"),
            P("expert", None, "mp"),
            P("expert", "mp", None),
            P("expert", "mp"),
            P("expert", None),
        ),
        out_specs=(P("expert", "mp"), P("expert", "mp", None), P("expert", "mp")),
        check_vma=False,
    )
```

```python
import functools
import math

import jax
import jax.numpy as jnp
from jax import lax
from jax.experimental import pallas as pl
from jax.experimental.pallas import tpu as pltpu
from jax.sharding import PartitionSpec as P

qmax = 7.0
wiggle = 0.9
two_pi = 6.283185307179586
F32 = jnp.float32
BF16 = jnp.bfloat16

SIN = (3.141592640130707, -5.167710083507862, 2.550077523214134, -0.5982912856178576, 0.0776576603009221)
COS = (0.9999999532476082, -4.93479283061961, 4.058411352862034, -1.3318765680776314, 0.2196896110917421)


def poly(z, coefs):
    total = coefs[-1] * z + coefs[-2]
    for coef in coefs[-3::-1]:
        total = total * z + coef
    return total


def quantize(w, step, inv7):
    t = w * inv7
    u = jnp.tanh(t)
    c = qmax * u
    r = c - jnp.floor(c + 0.5)
    z = r * r
    sine = r * poly(z, SIN)
    cosine = poly(z, COS)
    stair = c - (2.0 * wiggle / two_pi) * (sine * cosine)
    slopes = ((1.0 - wiggle) + (2.0 * wiggle) * (sine * sine)) * (1.0 - u * u)
    return step * stair, slopes, stair - (qmax * t) * slopes


def dot(a, b, ca, cb):
    return lax.dot_general(a, b, (((ca,), (cb,)), ((), ())), preferred_element_type=F32)


def upper(n):
    rows = lax.broadcasted_iota(jnp.int32, (n, n), 0)
    cols = lax.broadcasted_iota(jnp.int32, (n, n), 1)
    return jnp.where(rows < cols, 1.0, 0.0).astype(BF16)


def pack_kernel(cap, experts, ids_ref, cot_ref, out_ref):
    chunks = ids_ref.shape[0]
    ahead = upper(128)
    expert = lax.broadcasted_iota(jnp.int32, (experts, 128), 0)
    base = expert.astype(F32) * float(cap)
    seen = jnp.zeros((experts, 1), F32)
    slots = []
    for c in range(chunks):
        hot = jnp.where(expert == ids_ref[c : c + 1, :], 1.0, 0.0)
        place = dot(hot.astype(BF16), ahead, 1, 0) + seen + base
        slots.append(jnp.sum(hot * place, axis=0, keepdims=True))
        seen = seen + jnp.sum(hot, axis=1, keepdims=True)
    slot_row = jnp.concatenate(slots, axis=1).astype(jnp.int32)
    rows = lax.broadcasted_iota(jnp.int32, (128, chunks * 128), 0)
    for j in range(experts * cap // 128):
        pick = jnp.where(rows + 128 * j == slot_row, 1.0, 0.0).astype(BF16)
        out_ref[pl.ds(128 * j, 128), :] = dot(pick, cot_ref[...], 1, 0).astype(BF16)


def pack(ids_rows, cot, cap, experts):
    return pl.pallas_call(
        functools.partial(pack_kernel, cap, experts),
        out_shape=jax.ShapeDtypeStruct((experts * cap, cot.shape[1]), BF16),
        name="pack",
    )(ids_rows, cot)


TILE = 128
STEP_COLS = 512
STEP_ROWS = 16


def ring4(pos, device, view, send, recv):
    up, down, far = lax.rem(pos + 1, 4), lax.rem(pos + 3, 4), lax.rem(pos + 2, 4)

    def copy(src, k, part, k_to, n):
        return pltpu.make_async_remote_copy(
            src_ref=view(k, part) if src is None else src,
            dst_ref=view(k, part),
            send_sem=send.at[n],
            recv_sem=recv.at[n],
            device_id=device(k_to),
            device_id_type=pl.DeviceIdType.MESH,
        )

    class Ring:
        def start(self, src=None):
            copy(src, pos, "all", up, 0).start()
            copy(src, pos, "all", down, 1).start()

        def from_down(self):
            copy(None, down, "all", up, 0).wait_recv()
            copy(None, down, "lo", up, 2).start()

        def from_up(self):
            copy(None, up, "all", down, 1).wait_recv()
            copy(None, up, "hi", down, 3).start()

        def finish(self):
            copy(None, far, "lo", up, 2).wait_recv()
            copy(None, far, "hi", down, 3).wait_recv()

        def drain(self):
            copy(None, pos, "all", up, 0).wait_send()
            copy(None, pos, "all", down, 1).wait_send()
            copy(None, down, "lo", up, 2).wait_send()
            copy(None, up, "hi", down, 3).wait_send()

    return Ring()


def exchange_kernel(
    packed, tokens, ids, steps, weights,
    g, x, ids_all, q, slopes, step_slopes,
    steps_all, w_buf, o_buf,
    a2a_send, a2a_recv, pair_send, pair_recv, z_send, z_recv, x_send, x_recv,
    ids_send, ids_recv, steps_send, steps_recv, own_sem, w_sem, o_sem,
):
    me, part = lax.axis_index("expert"), lax.axis_index("mp")
    groups, parts = lax.axis_size("expert"), lax.axis_size("mp")
    row, col = me // 4, lax.rem(me, 4)
    z, core = part // 2, lax.rem(part, 2)
    width = packed.shape[-1]

    def remote(src, dst, send, recv, expert, mp):
        return pltpu.make_async_remote_copy(
            src_ref=src, dst_ref=dst, send_sem=send, recv_sem=recv,
            device_id=(expert, mp), device_id_type=pl.DeviceIdType.MESH,
        )

    barrier = pltpu.get_barrier_semaphore()
    for k in range(1, groups):
        pl.semaphore_signal(barrier, 1, device_id=(lax.rem(me + k, groups), part), device_id_type=pl.DeviceIdType.MESH)
    for k in range(1, parts):
        pl.semaphore_signal(barrier, 1, device_id=(me, lax.rem(part + k, parts)), device_id_type=pl.DeviceIdType.MESH)
    first_w = pltpu.make_async_copy(weights.at[0, pl.ds(0, TILE), :], w_buf.at[0], w_sem.at[0])
    first_w.start()

    def lanes(p):
        return pl.ds(pl.multiple_of(p * width, width), width)

    own_g = pltpu.make_async_copy(packed.at[me], g.at[:, me, :, lanes(part)], own_sem.at[0])
    own_x = pltpu.make_async_copy(tokens, x.at[row, col], own_sem.at[1])
    own_ids = pltpu.make_async_copy(ids, ids_all.at[me], own_sem.at[2])
    own_steps = pltpu.make_async_copy(steps, steps_all.at[part], own_sem.at[3])
    for own in (own_g, own_x, own_ids, own_steps):
        own.start()
    pl.semaphore_wait(barrier, groups + parts - 2)

    steps_sent = [
        remote(steps, steps_all.at[part], steps_send.at[k], steps_recv.at[k], me, lax.rem(part + k, parts))
        for k in range(1, parts)
    ]
    for copy in steps_sent:
        copy.start()

    def a2a(r, k):
        to = lax.rem(row - r + 4, 4) * 4 + lax.rem(col + k, 4)
        return remote(packed.at[to], g.at[:, me, :, lanes(part)], a2a_send.at[r, k], a2a_recv.at[r, k], to, part)

    def a2a_wait(r):
        for k in range(4):
            if r or k:
                source = lax.rem(row + r, 4) * 4 + lax.rem(col - k + 4, 4)
                remote(packed.at[source], g.at[:, source, :, lanes(part)], a2a_send.at[r, k], a2a_recv.at[r, k], source, part).wait_recv()

    pairs = [(r, k) for r in range(4) for k in range(4) if r or k]
    for r, k in pairs:
        a2a(r, k).start()

    ids_sent = [
        remote(ids, ids_all.at[me], ids_send.at[k], ids_recv.at[k], lax.rem(me + k, groups), part) for k in range(1, groups)
    ]
    for copy in ids_sent:
        copy.start()

    half = tokens.shape[0] // 2
    quarter = half // 2

    def on_x(k):
        return (row * 4 + k, part)

    def on_y(k):
        return (k * 4 + col, part)

    def x_rows(k, piece, base):
        return pl.ds(base + (quarter if piece == "hi" else 0), half if piece == "all" else quarter)

    def x_pair(piece):
        return pl.ds(2 if piece == "hi" else 0, 4 if piece == "all" else 2)

    x1a = ring4(col, on_x, lambda k, piece: x.at[row, k, x_rows(k, piece, 0)], x_send.at[0], x_recv.at[0])
    x1b = ring4(row, on_y, lambda k, piece: x.at[k, col, x_rows(k, piece, half)], x_send.at[1], x_recv.at[1])
    x2a = ring4(row, on_y, lambda k, piece: x.at[k, x_pair(piece), pl.ds(0, half)], x_send.at[2], x_recv.at[2])
    x2b = ring4(col, on_x, lambda k, piece: x.at[x_pair(piece), k, pl.ds(half, half)], x_send.at[3], x_recv.at[3])
    x1a.start(tokens.at[pl.ds(0, half)])
    x1b.start(tokens.at[pl.ds(half, half)])

    def on_z(k):
        return (me, k * 2 + core)

    def g_view(r, owner):
        sources = pl.ds(pl.multiple_of(lax.rem(row + r, 4) * 4, 4), 4)

        def view(k, piece):
            some = {"all": pl.ds(0, 2), "lo": pl.ds(0, 1), "hi": pl.ds(1, 1)}[piece]
            return g.at[some, sources, :, lanes(k * 2 + owner)]

        return view

    z_rings = [ring4(z, on_z, g_view(r, core), z_send.at[r], z_recv.at[r]) for r in range(4)]

    def to_pair(r, n):
        view = g_view(r, core)(lax.rem(z + (0, 3, 1, 2)[n], 4), "all")
        return remote(view, view, pair_send.at[r, n], pair_recv.at[r, n], me, z * 2 + 1 - core)

    def from_pair(r, n):
        view = g_view(r, 1 - core)(lax.rem(z + (0, 3, 1, 2)[n], 4), "all")
        return remote(view, view, pair_send.at[r, n], pair_recv.at[r, n], me, z * 2 + 1 - core)

    def arrive(r):
        def event():
            a2a_wait(r)
            if r == 0:
                own_g.wait()
            z_rings[r].start()
            to_pair(r, 0).start()

        return event

    def down(r):
        def event():
            z_rings[r].from_down()
            to_pair(r, 1).start()
            z_rings[r].from_up()
            to_pair(r, 2).start()

        return event

    def far(r):
        def event():
            z_rings[r].finish()
            to_pair(r, 3).start()

        return event

    def x_mid():
        for ring in (x1a, x1b):
            ring.from_down()
            ring.from_up()

    def x_second():
        own_x.wait()
        for ring, other in ((x1a, x2a), (x1b, x2b)):
            ring.finish()
            other.start()

    def x_mid2():
        for ring in (x2a, x2b):
            ring.from_down()
            ring.from_up()

    tiles_each = weights.shape[1] // TILE
    tiles = weights.shape[0] * tiles_each
    outs = (q, slopes, step_slopes)

    def w_in(t, slot):
        at = pl.ds(pl.multiple_of(lax.rem(t, tiles_each) * TILE, TILE), TILE)
        return pltpu.make_async_copy(weights.at[t // tiles_each, at, :], w_buf.at[slot], w_sem.at[slot])

    def q_out(t, slot, n):
        at = pl.ds(pl.multiple_of(lax.rem(t, tiles_each) * TILE, TILE), TILE)
        return pltpu.make_async_copy(o_buf.at[slot, n], outs[n].at[t // tiles_each, at, :], o_sem.at[slot, n])

    def tile(t, carry):
        slot = lax.rem(t, 2)
        w_in(t, slot).wait()

        @pl.when(t + 1 < tiles)
        def _():
            w_in(t + 1, 1 - slot).start()

        @pl.when(t >= 2)
        def _():
            for n in range(3):
                q_out(t - 2, slot, n).wait()

        e = t // tiles_each

        def chunk(j, carry):
            cols = pl.ds(pl.multiple_of(j * STEP_COLS, STEP_COLS), STEP_COLS)
            per = STEP_COLS // width
            s = jnp.concatenate([steps_all[j * per + n, pl.ds(e, 1), :] for n in range(per)], axis=1)
            inv7 = 1.0 / (qmax * s)

            def rows(k, carry):
                at = pl.ds(pl.multiple_of(k * STEP_ROWS, STEP_ROWS), STEP_ROWS)
                level, slope, step_slope = quantize(w_buf[slot, at, cols].astype(F32), s, inv7)
                o_buf[slot, 0, at, cols] = level.astype(BF16)
                o_buf[slot, 1, at, cols] = slope.astype(BF16)
                o_buf[slot, 2, at, cols] = step_slope.astype(BF16)
                return carry

            return lax.fori_loop(0, TILE // STEP_ROWS, rows, carry, unroll=2)

        lax.fori_loop(0, weights.shape[2] // STEP_COLS, chunk, 0)
        for n in range(3):
            q_out(t, slot, n).start()
        return carry

    own_steps.wait()
    for copy in steps_sent:
        copy.wait_recv()

    plan = (
        (1, arrive(0)), (3, arrive(1)), (5, arrive(2)), (6, down(0)), (7, arrive(3)), (8, x_mid), (9, down(1)),
        (10, x_second), (11, far(0)), (12, down(2)), (13, x_mid2), (14, far(1)), (14, down(3)), (14, far(2)), (14, far(3)),
    )
    done = 0
    for until, event in plan:
        if until > done:
            lax.fori_loop(done, until, tile, 0)
            done = until
        event()

    for t in (tiles - 2, tiles - 1):
        for n in range(3):
            q_out(t, t % 2, n).wait()
    for ring in (x2a, x2b):
        ring.finish()
    own_ids.wait()
    for copy in ids_sent:
        copy.wait_recv()
    for r in range(4):
        for n in range(4):
            from_pair(r, n).wait_recv()
    for copy in steps_sent + ids_sent:
        copy.wait_send()
    for r, k in pairs:
        a2a(r, k).wait_send()
    for ring in (x1a, x1b, x2a, x2b, *z_rings):
        ring.drain()
    for r in range(4):
        for n in range(4):
            to_pair(r, n).wait_send()


def exchange(packed, tokens, ids, steps, weights):
    groups, local, cap, part_f = packed.shape
    parts = lax.axis_size("mp")
    e, d, f = weights.shape
    toks, width = tokens.shape
    dma = pltpu.SemaphoreType.DMA
    vmem = pl.BlockSpec(memory_space=pltpu.VMEM)
    anywhere = pl.BlockSpec(memory_space=pl.ANY)
    return pl.pallas_call(
        exchange_kernel,
        in_specs=[vmem] * 4 + [anywhere],
        out_specs=[anywhere] * 6,
        out_shape=[
            jax.ShapeDtypeStruct((local, groups, cap, f), BF16),
            jax.ShapeDtypeStruct((4, groups // 4, toks, width), BF16),
            jax.ShapeDtypeStruct((groups, *ids.shape), jnp.int32),
            *[jax.ShapeDtypeStruct((e, d, f), BF16)] * 3,
        ],
        scratch_shapes=[
            pltpu.VMEM((parts, *steps.shape), F32),
            pltpu.VMEM((2, TILE, f), BF16),
            pltpu.VMEM((2, 3, TILE, f), BF16),
            dma((4, 4)), dma((4, 4)), dma((4, 4)), dma((4, 4)), dma((4, 4)), dma((4, 4)), dma((4, 4)), dma((4, 4)),
            dma((groups,)), dma((groups,)), dma((parts,)), dma((parts,)), dma((4,)), dma((2,)), dma((2, 3)),
        ],
        compiler_params=pltpu.CompilerParams(collective_id=0, has_side_effects=True),
        cost_estimate=pl.CostEstimate(flops=50 * e * d * f, bytes_accessed=60 << 20, transcendentals=e * d * f),
        name="exchange",
    )(packed, tokens, ids, steps, weights)


def selection(ids_ref, first, local, cap):
    groups, _, toks = ids_ref.shape
    ahead = upper(toks)
    picks = []
    for e in range(local):
        named = [jnp.max(jnp.where(ids_ref[i] == first + e, 1.0, 0.0), axis=0, keepdims=True) for i in range(groups)]
        named = jnp.concatenate(named, axis=0)
        place = dot(named.astype(BF16), ahead, 1, 0)
        picks.append(jnp.where(named > 0.0, place, -1.0).astype(jnp.int32))
    return picks


def pick_of(places, i, cap):
    slot = lax.broadcasted_iota(jnp.int32, (cap, places.shape[1]), 0)
    return jnp.where(slot == places[i : i + 1, :], 1.0, 0.0).astype(BF16)


def back_kernel(cap, ids_ref, g_ref, q_ref, out_ref, sums, backs):
    e = pl.program_id(0)
    local = pl.num_programs(0)
    groups = ids_ref.shape[0]
    g = g_ref[...].reshape(groups * cap, g_ref.shape[-1])
    backs[...] = dot(g, q_ref[0], 1, 1).astype(BF16)
    places = selection(ids_ref, lax.axis_index("expert") * local + e, 1, cap)[0]
    for i in range(groups):
        part = dot(pick_of(places, i, cap), backs[pl.ds(i * cap, cap), :], 0, 0)

        @pl.when(e == 0)
        def _():
            sums[i] = part

        @pl.when(e > 0)
        def _():
            out_ref[i] = (sums[i] + part).astype(BF16)


def back(ids, g, q):
    local, groups, cap, f = g.shape
    d = q.shape[1]
    toks = ids.shape[2]
    return pl.pallas_call(
        functools.partial(back_kernel, cap),
        grid=(local,),
        in_specs=[
            pl.BlockSpec(ids.shape, lambda e: (0, 0, 0)),
            pl.BlockSpec((1, groups, cap, f), lambda e: (e, 0, 0, 0)),
            pl.BlockSpec((1, d, f), lambda e: (e, 0, 0)),
        ],
        out_specs=pl.BlockSpec((groups, toks, d), lambda e: (0, 0, 0)),
        out_shape=jax.ShapeDtypeStruct((groups, toks, d), BF16),
        scratch_shapes=[pltpu.VMEM((groups, toks, d), F32), pltpu.VMEM((groups * cap, d), BF16)],
        cost_estimate=pl.CostEstimate(flops=2 * groups * local * cap * f * d, bytes_accessed=20 << 20, transcendentals=0),
        name="back",
    )(ids, g, q)


def raw_kernel(cap, ids_ref, x_ref, g_ref, a_ref, b_ref, w_ref, s_ref, picked):
    e = pl.program_id(0)
    local = pl.num_programs(0)
    groups = ids_ref.shape[0]

    @pl.when(pl.program_id(1) == 0)
    def _():
        places = selection(ids_ref, lax.axis_index("expert") * local + e, 1, cap)[0]
        for i in range(groups):
            part = dot(pick_of(places, i, cap), x_ref[i], 1, 0).astype(BF16)
            picked[:, pl.ds(i * cap, cap)] = part.T

    g = g_ref[...].reshape(groups * cap, g_ref.shape[-1])
    raw = dot(picked[...], g, 1, 0)
    w_ref[0] = (raw * a_ref[0].astype(F32)).astype(BF16)
    s_ref[0] = jnp.sum(raw * b_ref[0].astype(F32), axis=0, keepdims=True)


def raw_grads(ids, x, g, slopes, step_slopes):
    local, groups, cap, f = g.shape
    d = slopes.shape[1]
    tile = 256
    block = pl.BlockSpec((1, d, tile), lambda e, j: (e, 0, j))
    return pl.pallas_call(
        functools.partial(raw_kernel, cap),
        grid=(local, f // tile),
        in_specs=[
            pl.BlockSpec(ids.shape, lambda e, j: (0, 0, 0)),
            pl.BlockSpec(x.shape, lambda e, j: (0, 0, 0)),
            pl.BlockSpec((1, groups, cap, tile), lambda e, j: (e, 0, 0, j)),
            block,
            block,
        ],
        out_specs=[block, pl.BlockSpec((1, 1, tile), lambda e, j: (e, 0, j))],
        out_shape=[jax.ShapeDtypeStruct((local, d, f), BF16), jax.ShapeDtypeStruct((local, 1, f), F32)],
        scratch_shapes=[pltpu.VMEM((d, groups * cap), BF16)],
        cost_estimate=pl.CostEstimate(flops=2 * groups * local * cap * f * d, bytes_accessed=40 << 20, transcendentals=0),
        name="raw",
    )(ids, x, g, slopes, step_slopes)


def per_device(tokens, cotangent, weights, steps, expert_ids):
    groups = lax.axis_size("expert")
    parts = lax.axis_size("mp")
    local = weights.shape[0]
    experts = groups * local
    toks, top_k = expert_ids.shape
    cap = toks // 2
    width = tokens.shape[1]
    part_f = cotangent.shape[2]
    packed = pack(expert_ids.reshape(-1, 128), cotangent.reshape(toks * top_k, part_f), cap, experts)
    packed = packed.reshape(groups, local, cap, part_f)
    g, x, ids, q, slopes, step_slopes = exchange(packed, tokens, expert_ids.T, steps, weights)
    x = x.reshape(groups, toks, width)
    backs = back(ids, g, q)
    returned = lax.all_to_all(backs, "expert", split_axis=0, concat_axis=0, tiled=True)
    weight_out, partial_steps = raw_grads(ids, x, g, slopes, step_slopes)
    token_out = returned.astype(F32).sum(axis=0).astype(BF16)
    shares = partial_steps.reshape(local, parts, part_f).transpose(1, 0, 2)
    shares = lax.all_to_all(shares, "mp", split_axis=0, concat_axis=0, tiled=True)
    step_out = shares.sum(axis=0) * (1.0 / math.sqrt(width * parts * qmax))
    return (token_out, weight_out, step_out)


def solution(mesh):
    return jax.shard_map(
        per_device,
        mesh=mesh,
        in_specs=(
            P("expert", "mp"),
            P("expert", None, "mp"),
            P("expert", "mp", None),
            P("expert", "mp"),
            P("expert", None),
        ),
        out_specs=(P("expert", "mp"), P("expert", "mp", None), P("expert", "mp")),
        check_vma=False,
    )
```

```python
import functools
import math

import jax
import jax.numpy as jnp
from jax import lax
from jax.experimental import pallas as pl
from jax.experimental.pallas import tpu as pltpu
from jax.sharding import PartitionSpec as P

qmax = 7.0
wiggle = 0.9
two_pi = 6.283185307179586
F32 = jnp.float32
BF16 = jnp.bfloat16

ROOT = math.sqrt(2.0 * wiggle)
SIN = tuple(ROOT * c for c in (3.141592640130707, -5.167710083507862, 2.550077523214134, -0.5982912856178576, 0.0776576603009221))
COS = tuple(
    2.0 * wiggle / (two_pi * qmax * ROOT) * c
    for c in (0.9999999532476082, -4.93479283061961, 4.058411352862034, -1.3318765680776314, 0.2196896110917421)
)


def poly(z, coefs):
    total = coefs[-1] * z + coefs[-2]
    for coef in coefs[-3::-1]:
        total = total * z + coef
    return total


def quantize(w, step7, inv7):
    t = w * inv7
    u = jnp.tanh(t)
    c = qmax * u
    r = c - jnp.round(c)
    z = r * r
    sine = r * poly(z, SIN)
    stair = u - sine * poly(z, COS)
    slopes = ((1.0 - wiggle) + sine * sine) * (1.0 - u * u)
    return step7 * stair, slopes, stair - t * slopes


def dot(a, b, ca, cb):
    return lax.dot_general(a, b, (((ca,), (cb,)), ((), ())), preferred_element_type=F32)


def upper(n):
    rows = lax.broadcasted_iota(jnp.int32, (n, n), 0)
    cols = lax.broadcasted_iota(jnp.int32, (n, n), 1)
    return jnp.where(rows < cols, 1.0, 0.0).astype(BF16)


def slots_of(ids_ref, cap, experts):
    choices, toks = ids_ref.shape
    routes = choices * toks
    expert = lax.broadcasted_iota(jnp.int32, (experts, toks), 0)
    hot = [jnp.where(expert == ids_ref[k : k + 1, :], 1.0, 0.0) for k in range(choices)]
    place = dot(functools.reduce(jnp.add, hot).astype(BF16), upper(toks), 1, 0)
    places = [jnp.sum(one * place, axis=0, keepdims=True) for one in hot]
    both = jnp.concatenate([ids_ref[...].astype(F32), *places], axis=0).astype(BF16)
    token = lax.broadcasted_iota(jnp.int32, (toks, routes), 0)
    route = lax.broadcasted_iota(jnp.int32, (toks, routes), 1)
    spread = dot(both, jnp.where(route // choices == token, 1.0, 0.0).astype(BF16), 1, 0)
    slots = spread[:choices] * float(cap) + spread[choices:]
    choice = lax.broadcasted_iota(jnp.int32, (choices, routes), 0)
    mine = lax.rem(lax.broadcasted_iota(jnp.int32, (choices, routes), 1), choices) == choice
    return jnp.sum(jnp.where(mine, slots, 0.0), axis=0, keepdims=True).astype(jnp.int32)


def selection(ids_ref, first, local, cap):
    groups, _, toks = ids_ref.shape
    ahead = upper(toks)
    picks = []
    for e in range(local):
        named = [jnp.max(jnp.where(ids_ref[i] == first + e, 1.0, 0.0), axis=0, keepdims=True) for i in range(groups)]
        named = jnp.concatenate(named, axis=0)
        place = dot(named.astype(BF16), ahead, 1, 0)
        picks.append(jnp.where(named > 0.0, place, -1.0).astype(jnp.int32))
    return picks


TILE = 128
VMEM_LIMIT = 52 << 20
STEP_COLS = 512
STEP_ROWS = 16


def ring4(pos, device, view, send, recv):
    up, down, far = lax.rem(pos + 1, 4), lax.rem(pos + 3, 4), lax.rem(pos + 2, 4)

    def copy(src, k, part, k_to, n):
        return pltpu.make_async_remote_copy(
            src_ref=view(k, part) if src is None else src,
            dst_ref=view(k, part),
            send_sem=send.at[n],
            recv_sem=recv.at[n],
            device_id=device(k_to),
            device_id_type=pl.DeviceIdType.MESH,
        )

    class Ring:
        def start(self, src=None):
            copy(src, pos, "all", up, 0).start()
            copy(src, pos, "all", down, 1).start()

        def from_down(self):
            copy(None, down, "all", up, 0).wait_recv()
            copy(None, down, "lo", up, 2).start()

        def from_up(self):
            copy(None, up, "all", down, 1).wait_recv()
            copy(None, up, "hi", down, 3).start()

        def finish(self):
            copy(None, far, "lo", up, 2).wait_recv()
            copy(None, far, "hi", down, 3).wait_recv()

        def drain(self):
            copy(None, pos, "all", up, 0).wait_send()
            copy(None, pos, "all", down, 1).wait_send()
            copy(None, down, "lo", up, 2).wait_send()
            copy(None, up, "hi", down, 3).wait_send()

    return Ring()


def all4(pos, device, view, send, recv):
    def copy(k, owner):
        return pltpu.make_async_remote_copy(
            src_ref=view(owner),
            dst_ref=view(owner),
            send_sem=send.at[k],
            recv_sem=recv.at[k],
            device_id=device(lax.rem(pos + k, 4)),
            device_id_type=pl.DeviceIdType.MESH,
        )

    class Direct:
        def start(self):
            for k in (1, 3, 2):
                copy(k, pos).start()

        def finish(self):
            for k in range(1, 4):
                copy(k, lax.rem(pos - k + 4, 4)).wait_recv()

        def drain(self):
            for k in range(1, 4):
                copy(k, pos).wait_send()

    return Direct()


def layer_kernel(
    cap, cot, tokens, ids, steps, weights,
    token_out, weight_out, step_out,
    packed, g, x, ids_all, q, slopes, step_slopes, steps_all, w_buf,
    select, picked, backs, partial, got_1a, got_1b, got_2a, got_2b, sum_a, sum_b, token_t, step_parts, step_got,
    a2a_send, a2a_recv, pair_send, pair_recv, z_send, z_recv, x_send, x_recv,
    s1a_send, s1a_recv, s1b_send, s1b_recv, s2a_send, s2a_recv, s2b_send, s2b_recv,
    ids_send, ids_recv, steps_send, steps_recv, grads_send, grads_recv, own_sem, w_sem,
):
    me, part = lax.axis_index("expert"), lax.axis_index("mp")
    groups, parts = lax.axis_size("expert"), lax.axis_size("mp")
    row, col = me // 4, lax.rem(me, 4)
    z, core = part // 2, lax.rem(part, 2)
    width = cot.shape[-1]
    depth = tokens.shape[1]

    def remote(src, dst, send, recv, expert, mp):
        return pltpu.make_async_remote_copy(
            src_ref=src, dst_ref=dst, send_sem=send, recv_sem=recv,
            device_id=(expert, mp), device_id_type=pl.DeviceIdType.MESH,
        )

    barrier = pltpu.get_barrier_semaphore()
    for k in range(1, groups):
        pl.semaphore_signal(barrier, 1, device_id=(lax.rem(me + k, groups), part), device_id_type=pl.DeviceIdType.MESH)
    for k in range(1, parts):
        pl.semaphore_signal(barrier, 1, device_id=(me, lax.rem(part + k, parts)), device_id_type=pl.DeviceIdType.MESH)
    first_w = pltpu.make_async_copy(weights.at[0, pl.ds(0, TILE), :], w_buf.at[0], w_sem.at[0])
    first_w.start()

    def lanes(p):
        return pl.ds(pl.multiple_of(p * width, width), width)

    own_g = pltpu.make_async_copy(packed.at[me], g.at[:, me, :, lanes(part)], own_sem.at[0])
    own_ids = pltpu.make_async_copy(ids, ids_all.at[me], own_sem.at[2])
    own_steps = pltpu.make_async_copy(steps, steps_all.at[part], own_sem.at[3])
    for own in (own_ids, own_steps):
        own.start()

    x[row, col] = tokens[...].T
    slot_row = slots_of(ids, cap, groups * 2)
    slot = lax.broadcasted_iota(jnp.int32, (2 * cap, slot_row.shape[1]), 0)

    def pack(n, carry):
        to = lax.rem(row - n // 4 + 4, 4) * 4 + lax.rem(col + n, 4)
        pick = jnp.where(slot == slot_row - to * (2 * cap), 1.0, 0.0).astype(BF16)
        packed[to] = dot(pick, cot[...], 1, 0).astype(BF16).reshape(2, cap, width)
        return carry

    pl.semaphore_wait(barrier, groups + parts - 2)

    steps_sent = [
        remote(steps, steps_all.at[part], steps_send.at[k], steps_recv.at[k], me, lax.rem(part + k, parts))
        for k in range(1, parts)
    ]
    for copy in steps_sent:
        copy.start()

    def a2a(r, k):
        to = lax.rem(row - r + 4, 4) * 4 + lax.rem(col + k, 4)
        return remote(packed.at[to], g.at[:, me, :, lanes(part)], a2a_send.at[r, k], a2a_recv.at[r, k], to, part)

    def a2a_wait(r):
        for k in range(4):
            if r or k:
                source = lax.rem(row + r, 4) * 4 + lax.rem(col - k + 4, 4)
                remote(packed.at[source], g.at[:, source, :, lanes(part)], a2a_send.at[r, k], a2a_recv.at[r, k], source, part).wait_recv()

    half = depth // 2

    def on_x(k):
        return (row * 4 + k, part)

    def on_y(k):
        return (k * 4 + col, part)

    def x_pair(piece):
        return pl.ds(2 if piece == "hi" else 0, 4 if piece == "all" else 2)

    x1a = all4(col, on_x, lambda k: x.at[row, k, pl.ds(0, half)], x_send.at[0], x_recv.at[0])
    x1b = all4(row, on_y, lambda k: x.at[k, col, pl.ds(half, half)], x_send.at[1], x_recv.at[1])
    x2a = ring4(row, on_y, lambda k, piece: x.at[k, x_pair(piece), pl.ds(0, half)], x_send.at[2], x_recv.at[2])
    x2b = ring4(col, on_x, lambda k, piece: x.at[x_pair(piece), k, pl.ds(half, half)], x_send.at[3], x_recv.at[3])
    x1a.start()
    x1b.start()
    lax.fori_loop(0, groups // 2, pack, 0)
    own_g.start()
    pairs = [(r, k) for r in range(4) for k in range(4) if r or k]
    for r, k in pairs[:7]:
        a2a(r, k).start()
    ids_sent = [
        remote(ids, ids_all.at[me], ids_send.at[k], ids_recv.at[k], lax.rem(me + k, groups), part) for k in range(1, groups)
    ]
    for copy in ids_sent:
        copy.start()
    lax.fori_loop(groups // 2, groups, pack, 0)
    for r, k in pairs[7:]:
        a2a(r, k).start()

    def on_z(k):
        return (me, k * 2 + core)

    def g_view(r, owner):
        sources = pl.ds(pl.multiple_of(lax.rem(row + r, 4) * 4, 4), 4)

        def view(k, piece):
            some = {"all": pl.ds(0, 2), "lo": pl.ds(0, 1), "hi": pl.ds(1, 1)}[piece]
            return g.at[some, sources, :, lanes(k * 2 + owner)]

        return view

    z_rings = [ring4(z, on_z, g_view(r, core), z_send.at[r], z_recv.at[r]) for r in range(4)]

    def to_pair(r, n):
        view = g_view(r, core)(lax.rem(z + (0, 3, 1, 2)[n], 4), "all")
        return remote(view, view, pair_send.at[r, n], pair_recv.at[r, n], me, z * 2 + 1 - core)

    def from_pair(r, n):
        view = g_view(r, 1 - core)(lax.rem(z + (0, 3, 1, 2)[n], 4), "all")
        return remote(view, view, pair_send.at[r, n], pair_recv.at[r, n], me, z * 2 + 1 - core)

    def arrive(r):
        def event():
            a2a_wait(r)
            if r == 0:
                own_g.wait()
            z_rings[r].start()
            to_pair(r, 0).start()

        return event

    def down(r):
        def event():
            z_rings[r].from_down()
            to_pair(r, 1).start()
            z_rings[r].from_up()
            to_pair(r, 2).start()

        return event

    def far(r):
        def event():
            z_rings[r].finish()
            to_pair(r, 3).start()

        return event

    def x_second():
        for ring, other in ((x1a, x2a), (x1b, x2b)):
            ring.finish()
            other.start()

    def x_mid2():
        for ring in (x2a, x2b):
            ring.from_down()
            ring.from_up()

    tiles_each = weights.shape[1] // TILE
    tiles = weights.shape[0] * tiles_each

    def w_in(t, slot):
        at = pl.ds(pl.multiple_of(lax.rem(t, tiles_each) * TILE, TILE), TILE)
        return pltpu.make_async_copy(weights.at[t // tiles_each, at, :], w_buf.at[slot], w_sem.at[slot])

    def tile(t, carry):
        slot = lax.rem(t, 2)
        w_in(t, slot).wait()

        @pl.when(t + 1 < tiles)
        def _():
            w_in(t + 1, 1 - slot).start()

        e = t // tiles_each
        head = lax.rem(t, tiles_each) * TILE

        def chunk(j, carry):
            cols = pl.ds(pl.multiple_of(j * STEP_COLS, STEP_COLS), STEP_COLS)
            per = STEP_COLS // width
            s = jnp.concatenate([steps_all[j * per + n, pl.ds(e, 1), :] for n in range(per)], axis=1)
            step7 = qmax * s
            inv7 = 1.0 / step7

            def rows(k, carry):
                at = pl.ds(pl.multiple_of(k * STEP_ROWS, STEP_ROWS), STEP_ROWS)
                to = pl.ds(pl.multiple_of(head + k * STEP_ROWS, STEP_ROWS), STEP_ROWS)
                level, slope, step_slope = quantize(w_buf[slot, at, cols].astype(F32), step7, inv7)
                q[e, to, cols] = level.astype(BF16)
                slopes[e, to, cols] = slope.astype(BF16)
                step_slopes[e, to, cols] = step_slope.astype(BF16)
                return carry

            return lax.fori_loop(0, TILE // STEP_ROWS, rows, carry, unroll=2)

        lax.fori_loop(0, weights.shape[2] // STEP_COLS, chunk, 0)
        return carry

    top = sum_a.shape[1]
    bottom = depth - top

    def block_rows(r):
        return pl.multiple_of(lax.rem(row + r, 4) * 4, 4)

    def arrived(r):
        for n in range(4):
            from_pair(r, n).wait_recv()

    def selections():
        own_ids.wait()
        for copy in ids_sent:
            copy.wait_recv()
        places = selection(ids_all, me * 2, 2, cap)
        slot = lax.broadcasted_iota(jnp.int32, (2 * cap, 2 * ids.shape[1]), 0)
        for e in range(2):
            for n in range(groups // 2):
                first, second = places[e][2 * n : 2 * n + 1], places[e][2 * n + 1 : 2 * n + 2]
                place = jnp.concatenate([first, jnp.where(second < 0, second, second + cap)], axis=1)
                select[n, pl.ds(e * 2 * cap, 2 * cap)] = jnp.where(slot == place, 1.0, 0.0).astype(BF16)

    def picks():
        def one(n, carry):
            both = jnp.concatenate([x[n // 2, 2 * lax.rem(n, 2)], x[n // 2, 2 * lax.rem(n, 2) + 1]], axis=1)
            out = dot(both, select[n], 1, 1).astype(BF16)
            at = pl.ds(pl.multiple_of(n * 2 * cap, 2 * cap), 2 * cap)
            for e in range(2):
                picked[e, :, at] = out[:, 2 * cap * e : 2 * cap * (e + 1)]
            return carry

        lax.fori_loop(0, groups // 2, one, 0)

    def back(r):
        base = block_rows(r)
        for e in range(2):
            backs[e] = dot(q[e], g[e, pl.ds(base, 4)].reshape(4 * cap, -1), 1, 1).astype(BF16)
        for n in range(2):
            both = jnp.concatenate([backs[e, :, 2 * cap * n : 2 * cap * (n + 1)] for e in range(2)], axis=1)
            out = dot(both, select[base // 2 + n], 1, 0).astype(BF16)
            for k in range(2):
                partial[r, 2 * n + k] = out[:, 2 * cap * k : 2 * cap * (k + 1)]

    def s1a(r, k):
        to = lax.rem(col + k, 4)
        return remote(
            partial.at[r, to, pl.ds(0, top)], got_1a.at[r, k - 1], s1a_send.at[r, k], s1a_recv.at[r, k], row * 4 + to, part
        )

    def s1b(r):
        to = lax.rem(row + r, 4)
        return remote(
            partial.at[r, :, pl.ds(top, bottom)], got_1b.at[r - 1], s1b_send.at[r], s1b_recv.at[r], to * 4 + col, part
        )

    def s2a(r):
        to = lax.rem(row + r, 4)
        return remote(sum_a.at[r - 1], got_2a.at[r - 1], s2a_send.at[r], s2a_recv.at[r], to * 4 + col, part)

    def s2b(k):
        to = lax.rem(col + k, 4)
        return remote(sum_b.at[k - 1], got_2b.at[k - 1], s2b_send.at[k], s2b_recv.at[k], row * 4 + to, part)

    def send_first(r):
        for k in range(1, 4):
            s1a(r, k).start()
        if r:
            s1b(r).start()

    def upper_sum(r):
        for k in range(1, 4):
            s1a(r, k).wait_recv()
        total = partial[r, col, pl.ds(0, top)].astype(F32)
        for k in range(3):
            total = total + got_1a[r, k].astype(F32)
        return total

    def second_a(r):
        sum_a[r - 1] = upper_sum(r).astype(BF16)

    def lower_sum(k):
        to = lax.rem(col + k, 4)
        total = partial[0, to, pl.ds(top, bottom)].astype(F32)
        for r in range(3):
            total = total + got_1b[r, to].astype(F32)
        return total

    def second_b():
        for r in range(1, 4):
            s1b(r).wait_recv()
        for k in range(1, 4):
            sum_b[k - 1] = lower_sum(k).astype(BF16)

    def grads(k):
        to = lax.rem(part + k, parts)
        return remote(step_parts.at[to], step_got.at[k - 1], grads_send.at[k], grads_recv.at[k], me, to)

    def raw(n, carry):
        p = lax.rem(part + 1 + n, parts)
        cols = lanes(p)

        for e in range(2):
            value = dot(picked[e], g[e, :, :, cols].reshape(groups * cap, width), 1, 0)
            weight_out[e, :, cols] = (value * slopes[e, :, cols].astype(F32)).astype(BF16)
            step_parts[p, pl.ds(e, 1), :] = jnp.sum(value * step_slopes[e, :, cols].astype(F32), axis=0, keepdims=True)
        @pl.when(n > 0)
        def _():
            grads(n).start()

        return carry

    own_steps.wait()
    for copy in steps_sent:
        copy.wait_recv()

    plan = (
        (2, x_second), (4, arrive(0)), (6, arrive(1)), (9, down(0)), (10, arrive(2)), (12, down(1)), (12, arrive(3)),
    )
    done = 0
    for until, event in plan:
        if until > done:
            lax.fori_loop(done, until, tile, 0)
            done = until
        event()
    lax.fori_loop(done, tiles, tile, 0)

    selections()
    far(0)()
    x_mid2()
    arrived(0)
    back(0)
    send_first(0)
    down(2)()
    far(1)()
    arrived(1)
    back(1)
    send_first(1)
    for ring in (x2a, x2b):
        ring.finish()
    down(3)()
    picks()
    far(2)()
    arrived(2)
    back(2)
    send_first(2)
    far(3)()
    arrived(3)
    back(3)
    send_first(3)
    second_a(1)
    lax.fori_loop(0, 1, raw, 0)
    s2a(1).start()
    lax.fori_loop(1, 5, raw, 0)
    second_a(2)
    lax.fori_loop(5, 6, raw, 0)
    s2a(2).start()
    lax.fori_loop(6, parts, raw, 0)
    second_a(3)
    s2a(3).start()
    second_b()
    upper = upper_sum(0)
    for k in range(1, 4):
        s2b(k).start()
    for r in range(1, 4):
        s2a(r).wait_recv()
        upper = upper + got_2a[r - 1].astype(F32)
    token_t[pl.ds(0, top)] = upper.astype(BF16)
    total = lower_sum(0)
    for k in range(1, 4):
        s2b(k).wait_recv()
        total = total + got_2b[k - 1].astype(F32)
    token_t[pl.ds(top, bottom)] = total.astype(BF16)
    token_out[...] = token_t[...].T
    total = step_parts[part]
    for k in range(1, parts):
        grads(k).wait_recv()
        total = total + step_got[k - 1]
    step_out[...] = total * (qmax / math.sqrt(depth * parts * qmax))

    for copy in steps_sent + ids_sent:
        copy.wait_send()
    for r, k in pairs:
        a2a(r, k).wait_send()
    for ring in (x1a, x1b, x2a, x2b, *z_rings):
        ring.drain()
    for r in range(4):
        for n in range(4):
            to_pair(r, n).wait_send()
    for k in range(1, 4):
        for r in range(4):
            s1a(r, k).wait_send()
        s1b(k).wait_send()
        s2a(k).wait_send()
        s2b(k).wait_send()
    for k in range(1, parts):
        grads(k).wait_send()


def layer(cot, tokens, ids, steps, weights):
    groups, parts = lax.axis_size("expert"), lax.axis_size("mp")
    e, d, f = weights.shape
    toks, width = tokens.shape
    cap, part_f = toks // 2, cot.shape[1]
    top = d * 5 // 8 // 16 * 16
    bottom = d - top
    dma = pltpu.SemaphoreType.DMA
    vmem = pl.BlockSpec(memory_space=pltpu.VMEM)
    anywhere = pl.BlockSpec(memory_space=pl.ANY)
    slots = e * cap

    def room(*shape, dtype=BF16):
        return pltpu.VMEM(shape, dtype)

    return pl.pallas_call(
        functools.partial(layer_kernel, cap),
        in_specs=[vmem] * 4 + [anywhere],
        out_specs=[vmem, vmem, vmem],
        out_shape=[
            pltpu.VMEM((toks, width), BF16),
            pltpu.VMEM((e, d, f), BF16),
            pltpu.VMEM((e, part_f), F32),
        ],
        scratch_shapes=[
            room(groups, e, cap, part_f),
            room(e, groups, cap, f),
            room(4, groups // 4, d, toks),
            room(groups, *ids.shape, dtype=jnp.int32),
            room(e, d, f), room(e, d, f), room(e, d, f),
            room(parts, *steps.shape, dtype=F32),
            room(2, TILE, f),
            room(groups // 2, 2 * slots, 2 * toks),
            room(e, d, groups * cap),
            room(e, d, 4 * cap),
            room(4, 4, d, toks),
            room(4, 3, top, toks),
            room(3, 4, bottom, toks),
            room(3, top, toks), room(3, bottom, toks), room(3, top, toks), room(3, bottom, toks),
            room(d, toks),
            room(parts, e, part_f, dtype=F32),
            room(parts - 1, e, part_f, dtype=F32),
            *[dma((4, 4))] * 8,
            *[dma((4, 4))] * 2, *[dma((4,))] * 6,
            dma((groups,)), dma((groups,)), dma((parts,)), dma((parts,)), dma((parts,)), dma((parts,)),
            dma((4,)), dma((2,)),
        ],
        compiler_params=pltpu.CompilerParams(collective_id=0, has_side_effects=True, vmem_limit_bytes=VMEM_LIMIT),
        name="layer",
    )(cot, tokens, ids, steps, weights)


def per_device(tokens, cotangent, weights, steps, expert_ids):
    toks, top_k = expert_ids.shape
    cot = cotangent.reshape(toks * top_k, cotangent.shape[2])
    return tuple(layer(cot, tokens, expert_ids.T, steps, weights))


def solution(mesh):
    return jax.shard_map(
        per_device,
        mesh=mesh,
        in_specs=(
            P("expert", "mp"),
            P("expert", None, "mp"),
            P("expert", "mp", None),
            P("expert", "mp"),
            P("expert", None),
        ),
        out_specs=(P("expert", "mp"), P("expert", "mp", None), P("expert", "mp")),
        check_vma=False,
    )
```

```python
import functools
import math

import jax
import jax.numpy as jnp
from jax import lax
from jax.experimental import pallas as pl
from jax.experimental.pallas import tpu as pltpu
from jax.sharding import PartitionSpec as P

qmax = 7.0
wiggle = 0.9
two_pi = 6.283185307179586
F32 = jnp.float32
BF16 = jnp.bfloat16

ROOT = math.sqrt(2.0 * wiggle)
SIN = tuple(ROOT * c for c in (3.141592640130707, -5.167710083507862, 2.550077523214134, -0.5982912856178576, 0.0776576603009221))
COS = tuple(
    2.0 * wiggle / (two_pi * qmax * ROOT) * c
    for c in (0.9999999532476082, -4.93479283061961, 4.058411352862034, -1.3318765680776314, 0.2196896110917421)
)


def poly(z, coefs):
    total = coefs[-1] * z + coefs[-2]
    for coef in coefs[-3::-1]:
        total = total * z + coef
    return total


def quantize(w, step7, inv7):
    t = w * inv7
    u = jnp.tanh(t)
    c = qmax * u
    r = c - jnp.round(c)
    z = r * r
    sine = r * poly(z, SIN)
    stair = u - sine * poly(z, COS)
    slopes = ((1.0 - wiggle) + sine * sine) * (1.0 - u * u)
    return step7 * stair, slopes, stair - t * slopes


def dot(a, b, ca, cb):
    return lax.dot_general(a, b, (((ca,), (cb,)), ((), ())), preferred_element_type=F32)


def upper(n):
    rows = lax.broadcasted_iota(jnp.int32, (n, n), 0)
    cols = lax.broadcasted_iota(jnp.int32, (n, n), 1)
    return jnp.where(rows < cols, 1.0, 0.0).astype(BF16)


def slots_of(ids_ref, cap, experts):
    choices, toks = ids_ref.shape
    routes = choices * toks
    expert = lax.broadcasted_iota(jnp.int32, (experts, toks), 0)
    hot = [jnp.where(expert == ids_ref[k : k + 1, :], 1.0, 0.0) for k in range(choices)]
    place = dot(functools.reduce(jnp.add, hot).astype(BF16), upper(toks), 1, 0)
    places = [jnp.sum(one * place, axis=0, keepdims=True) for one in hot]
    both = jnp.concatenate([ids_ref[...].astype(F32), *places], axis=0).astype(BF16)
    token = lax.broadcasted_iota(jnp.int32, (toks, routes), 0)
    route = lax.broadcasted_iota(jnp.int32, (toks, routes), 1)
    spread = dot(both, jnp.where(route // choices == token, 1.0, 0.0).astype(BF16), 1, 0)
    slots = spread[:choices] * float(cap) + spread[choices:]
    choice = lax.broadcasted_iota(jnp.int32, (choices, routes), 0)
    mine = lax.rem(lax.broadcasted_iota(jnp.int32, (choices, routes), 1), choices) == choice
    return jnp.sum(jnp.where(mine, slots, 0.0), axis=0, keepdims=True).astype(jnp.int32)


def selection(ids_ref, first, local, cap):
    groups, _, toks = ids_ref.shape
    ahead = upper(toks)
    picks = []
    for e in range(local):
        named = [jnp.max(jnp.where(ids_ref[i] == first + e, 1.0, 0.0), axis=0, keepdims=True) for i in range(groups)]
        named = jnp.concatenate(named, axis=0)
        place = dot(named.astype(BF16), ahead, 1, 0)
        picks.append(jnp.where(named > 0.0, place, -1.0).astype(jnp.int32))
    return picks


TILE = 128
VMEM_LIMIT = 52 << 20
STEP_COLS = 512
STEP_ROWS = 16


def ring4(pos, device, view, send, recv):
    up, down, far = lax.rem(pos + 1, 4), lax.rem(pos + 3, 4), lax.rem(pos + 2, 4)

    def copy(src, k, part, k_to, n):
        return pltpu.make_async_remote_copy(
            src_ref=view(k, part) if src is None else src,
            dst_ref=view(k, part),
            send_sem=send.at[n],
            recv_sem=recv.at[n],
            device_id=device(k_to),
            device_id_type=pl.DeviceIdType.MESH,
        )

    class Ring:
        def start(self, src=None):
            copy(src, pos, "all", up, 0).start()
            copy(src, pos, "all", down, 1).start()

        def from_down(self):
            copy(None, down, "all", up, 0).wait_recv()
            copy(None, down, "lo", up, 2).start()

        def from_up(self):
            copy(None, up, "all", down, 1).wait_recv()
            copy(None, up, "hi", down, 3).start()

        def finish(self):
            copy(None, far, "lo", up, 2).wait_recv()
            copy(None, far, "hi", down, 3).wait_recv()

        def drain(self):
            copy(None, pos, "all", up, 0).wait_send()
            copy(None, pos, "all", down, 1).wait_send()
            copy(None, down, "lo", up, 2).wait_send()
            copy(None, up, "hi", down, 3).wait_send()

    return Ring()


def all4(pos, device, view, send, recv):
    def copy(k, owner):
        return pltpu.make_async_remote_copy(
            src_ref=view(owner),
            dst_ref=view(owner),
            send_sem=send.at[k],
            recv_sem=recv.at[k],
            device_id=device(lax.rem(pos + k, 4)),
            device_id_type=pl.DeviceIdType.MESH,
        )

    class Direct:
        def start(self):
            for k in (1, 3, 2):
                copy(k, pos).start()

        def finish(self):
            for k in range(1, 4):
                copy(k, lax.rem(pos - k + 4, 4)).wait_recv()

        def drain(self):
            for k in range(1, 4):
                copy(k, pos).wait_send()

    return Direct()


def layer_kernel(
    cap, cot, tokens, ids, steps, weights,
    token_out, weight_out, step_out,
    packed, g, x, ids_all, q, slopes, step_slopes, steps_all, w_buf,
    select, picked, backs, partial, got_1a, got_1b, got_2a, got_2b, sum_a, sum_b, token_t, step_parts, step_got,
    a2a_send, a2a_recv, pair_send, pair_recv, z_send, z_recv, x_send, x_recv,
    s1a_send, s1a_recv, s1b_send, s1b_recv, s2a_send, s2a_recv, s2b_send, s2b_recv,
    ids_send, ids_recv, steps_send, steps_recv, grads_send, grads_recv, own_sem, w_sem,
):
    me, part = lax.axis_index("expert"), lax.axis_index("mp")
    groups, parts = lax.axis_size("expert"), lax.axis_size("mp")
    row, col = me // 4, lax.rem(me, 4)
    z, core = part // 2, lax.rem(part, 2)
    width = cot.shape[-1]
    depth = tokens.shape[1]

    def remote(src, dst, send, recv, expert, mp):
        return pltpu.make_async_remote_copy(
            src_ref=src, dst_ref=dst, send_sem=send, recv_sem=recv,
            device_id=(expert, mp), device_id_type=pl.DeviceIdType.MESH,
        )

    barrier = pltpu.get_barrier_semaphore()
    for k in range(1, groups):
        pl.semaphore_signal(barrier, 1, device_id=(lax.rem(me + k, groups), part), device_id_type=pl.DeviceIdType.MESH)
    for k in range(1, parts):
        pl.semaphore_signal(barrier, 1, device_id=(me, lax.rem(part + k, parts)), device_id_type=pl.DeviceIdType.MESH)
    first_w = pltpu.make_async_copy(weights.at[0, pl.ds(0, TILE), :], w_buf.at[0], w_sem.at[0])
    first_w.start()

    def lanes(p):
        return pl.ds(pl.multiple_of(p * width, width), width)

    own_g = pltpu.make_async_copy(packed.at[me], g.at[:, me, :, lanes(part)], own_sem.at[0])
    own_ids = pltpu.make_async_copy(ids, ids_all.at[me], own_sem.at[2])
    own_steps = pltpu.make_async_copy(steps, steps_all.at[part], own_sem.at[3])
    for own in (own_ids, own_steps):
        own.start()

    x[row, col] = tokens[...].T
    slot_row = slots_of(ids, cap, groups * 2)
    slot = lax.broadcasted_iota(jnp.int32, (2 * cap, slot_row.shape[1]), 0)

    def pack(n, carry):
        to = lax.rem(row - n // 4 + 4, 4) * 4 + lax.rem(col + n, 4)
        pick = jnp.where(slot == slot_row - to * (2 * cap), 1.0, 0.0).astype(BF16)
        packed[to] = dot(pick, cot[...], 1, 0).astype(BF16).reshape(2, cap, width)
        return carry

    pl.semaphore_wait(barrier, groups + parts - 2)

    steps_sent = [
        remote(steps, steps_all.at[part], steps_send.at[k], steps_recv.at[k], me, lax.rem(part + k, parts))
        for k in range(1, parts)
    ]
    for copy in steps_sent:
        copy.start()

    def a2a(r, k):
        to = lax.rem(row - r + 4, 4) * 4 + lax.rem(col + k, 4)
        return remote(packed.at[to], g.at[:, me, :, lanes(part)], a2a_send.at[r, k], a2a_recv.at[r, k], to, part)

    def a2a_wait(r):
        for k in range(4):
            if r or k:
                source = lax.rem(row + r, 4) * 4 + lax.rem(col - k + 4, 4)
                remote(packed.at[source], g.at[:, source, :, lanes(part)], a2a_send.at[r, k], a2a_recv.at[r, k], source, part).wait_recv()

    half = depth // 2

    def on_x(k):
        return (row * 4 + k, part)

    def on_y(k):
        return (k * 4 + col, part)

    def x_pair(piece):
        return pl.ds(2 if piece == "hi" else 0, 4 if piece == "all" else 2)

    x1a = all4(col, on_x, lambda k: x.at[row, k, pl.ds(0, half)], x_send.at[0], x_recv.at[0])
    x1b = all4(row, on_y, lambda k: x.at[k, col, pl.ds(half, half)], x_send.at[1], x_recv.at[1])
    x2a = ring4(row, on_y, lambda k, piece: x.at[k, x_pair(piece), pl.ds(0, half)], x_send.at[2], x_recv.at[2])
    x2b = ring4(col, on_x, lambda k, piece: x.at[x_pair(piece), k, pl.ds(half, half)], x_send.at[3], x_recv.at[3])
    x1a.start()
    x1b.start()
    lax.fori_loop(0, groups // 2, pack, 0)
    own_g.start()
    pairs = [(r, k) for r in range(4) for k in range(4) if r or k]
    for r, k in pairs[:7]:
        a2a(r, k).start()
    ids_sent = [
        remote(ids, ids_all.at[me], ids_send.at[k], ids_recv.at[k], lax.rem(me + k, groups), part) for k in range(1, groups)
    ]
    for copy in ids_sent:
        copy.start()
    lax.fori_loop(groups // 2, groups, pack, 0)
    for r, k in pairs[7:]:
        a2a(r, k).start()

    def on_z(k):
        return (me, k * 2 + core)

    def g_view(r, owner):
        sources = pl.ds(pl.multiple_of(lax.rem(row + r, 4) * 4, 4), 4)

        def view(k, piece):
            some = {"all": pl.ds(0, 2), "lo": pl.ds(0, 1), "hi": pl.ds(1, 1)}[piece]
            return g.at[some, sources, :, lanes(k * 2 + owner)]

        return view

    z_rings = [ring4(z, on_z, g_view(r, core), z_send.at[r], z_recv.at[r]) for r in range(4)]

    def to_pair(r, n):
        view = g_view(r, core)(lax.rem(z + (0, 3, 1, 2)[n], 4), "all")
        return remote(view, view, pair_send.at[r, n], pair_recv.at[r, n], me, z * 2 + 1 - core)

    def from_pair(r, n):
        view = g_view(r, 1 - core)(lax.rem(z + (0, 3, 1, 2)[n], 4), "all")
        return remote(view, view, pair_send.at[r, n], pair_recv.at[r, n], me, z * 2 + 1 - core)

    def arrive(r):
        def event():
            a2a_wait(r)
            if r == 0:
                own_g.wait()
            z_rings[r].start()
            to_pair(r, 0).start()

        return event

    def down(r):
        def event():
            z_rings[r].from_down()
            to_pair(r, 1).start()
            z_rings[r].from_up()
            to_pair(r, 2).start()

        return event

    def far(r):
        def event():
            z_rings[r].finish()
            to_pair(r, 3).start()

        return event

    def x_second():
        for ring, other in ((x1a, x2a), (x1b, x2b)):
            ring.finish()
            other.start()

    def x_mid2():
        for ring in (x2a, x2b):
            ring.from_down()
            ring.from_up()

    tiles_each = weights.shape[1] // TILE
    tiles = weights.shape[0] * tiles_each

    def w_in(t, slot):
        at = pl.ds(pl.multiple_of(lax.rem(t, tiles_each) * TILE, TILE), TILE)
        return pltpu.make_async_copy(weights.at[t // tiles_each, at, :], w_buf.at[slot], w_sem.at[slot])

    def tile(t, carry):
        slot = lax.rem(t, 2)
        w_in(t, slot).wait()

        @pl.when(t + 1 < tiles)
        def _():
            w_in(t + 1, 1 - slot).start()

        e = t // tiles_each
        head = lax.rem(t, tiles_each) * TILE

        def chunk(j, carry):
            cols = pl.ds(pl.multiple_of(j * STEP_COLS, STEP_COLS), STEP_COLS)
            per = STEP_COLS // width
            s = jnp.concatenate([steps_all[j * per + n, pl.ds(e, 1), :] for n in range(per)], axis=1)
            step7 = qmax * s
            inv7 = 1.0 / step7

            def rows(k, carry):
                at = pl.ds(pl.multiple_of(k * STEP_ROWS, STEP_ROWS), STEP_ROWS)
                to = pl.ds(pl.multiple_of(head + k * STEP_ROWS, STEP_ROWS), STEP_ROWS)
                level, slope, step_slope = quantize(w_buf[slot, at, cols].astype(F32), step7, inv7)
                q[e, to, cols] = level.astype(BF16)
                slopes[e, to, cols] = slope.astype(BF16)
                step_slopes[e, to, cols] = step_slope.astype(BF16)
                return carry

            return lax.fori_loop(0, TILE // STEP_ROWS, rows, carry, unroll=2)

        lax.fori_loop(0, weights.shape[2] // STEP_COLS, chunk, 0)
        return carry

    top = sum_a.shape[1]
    bottom = depth - top

    def block_rows(r):
        return pl.multiple_of(lax.rem(row + r, 4) * 4, 4)

    def arrived(r):
        for n in range(4):
            from_pair(r, n).wait_recv()

    def selections():
        own_ids.wait()
        for copy in ids_sent:
            copy.wait_recv()
        places = selection(ids_all, me * 2, 2, cap)
        slot = lax.broadcasted_iota(jnp.int32, (2 * cap, 2 * ids.shape[1]), 0)
        for e in range(2):
            for n in range(groups // 2):
                first, second = places[e][2 * n : 2 * n + 1], places[e][2 * n + 1 : 2 * n + 2]
                place = jnp.concatenate([first, jnp.where(second < 0, second, second + cap)], axis=1)
                select[n, pl.ds(e * 2 * cap, 2 * cap)] = jnp.where(slot == place, 1.0, 0.0).astype(BF16)

    def picks():
        def one(n, carry):
            both = jnp.concatenate([x[n // 2, 2 * lax.rem(n, 2)], x[n // 2, 2 * lax.rem(n, 2) + 1]], axis=1)
            out = dot(both, select[n], 1, 1).astype(BF16)
            at = pl.ds(pl.multiple_of(n * 2 * cap, 2 * cap), 2 * cap)
            for e in range(2):
                picked[e, :, at] = out[:, 2 * cap * e : 2 * cap * (e + 1)]
            return carry

        lax.fori_loop(0, groups // 2, one, 0)

    def back(r):
        base = block_rows(r)
        for e in range(2):
            backs[e] = dot(q[e], g[e, pl.ds(base, 4)].reshape(4 * cap, -1), 1, 1).astype(BF16)
        for n in range(2):
            both = jnp.concatenate([backs[e, :, 2 * cap * n : 2 * cap * (n + 1)] for e in range(2)], axis=1)
            out = dot(both, select[base // 2 + n], 1, 0).astype(BF16)
            for k in range(2):
                partial[r, 2 * n + k] = out[:, 2 * cap * k : 2 * cap * (k + 1)]

    cut = top // 32 * 16

    def piece(r, c):
        if r < 3:
            return pl.ds(0, top)
        return pl.ds(cut, top - cut) if c else pl.ds(0, cut)

    def s1a(r, k, c=0):
        to = lax.rem(col + k, 4)
        return remote(
            partial.at[r, to, piece(r, c)], got_1a.at[r, k - 1, piece(r, c)], s1a_send.at[r + c, k], s1a_recv.at[r + c, k],
            row * 4 + to, part,
        )

    def s1b(r):
        to = lax.rem(row + r, 4)
        return remote(
            partial.at[r, :, pl.ds(top, bottom)], got_1b.at[r - 1], s1b_send.at[r], s1b_recv.at[r], to * 4 + col, part
        )

    def s2a(r, c=0):
        to = lax.rem(row + r, 4)
        n = 0 if c else r
        return remote(
            sum_a.at[r - 1, piece(r, c)], got_2a.at[r - 1, piece(r, c)], s2a_send.at[n], s2a_recv.at[n], to * 4 + col, part
        )

    def s2b(k):
        to = lax.rem(col + k, 4)
        return remote(sum_b.at[k - 1], got_2b.at[k - 1], s2b_send.at[k], s2b_recv.at[k], row * 4 + to, part)

    def send_first(r):
        for c in range(2 if r == 3 else 1):
            for k in range(1, 4):
                s1a(r, k, c).start()
        if r:
            s1b(r).start()

    def upper_sum(r, c=0):
        for k in range(1, 4):
            s1a(r, k, c).wait_recv()
        total = partial[r, col, piece(r, c)].astype(F32)
        for k in range(3):
            total = total + got_1a[r, k, piece(r, c)].astype(F32)
        return total

    def second_a(r, c=0):
        sum_a[r - 1, piece(r, c)] = upper_sum(r, c).astype(BF16)

    def lower_sum(k):
        to = lax.rem(col + k, 4)
        total = partial[0, to, pl.ds(top, bottom)].astype(F32)
        for r in range(3):
            total = total + got_1b[r, to].astype(F32)
        return total

    def second_b():
        for r in range(1, 4):
            s1b(r).wait_recv()
        for k in range(1, 4):
            sum_b[k - 1] = lower_sum(k).astype(BF16)

    def grads(k):
        to = lax.rem(part + k, parts)
        return remote(step_parts.at[to], step_got.at[k - 1], grads_send.at[k], grads_recv.at[k], me, to)

    def raw(n, carry):
        p = lax.rem(part + 1 + n, parts)
        cols = lanes(p)

        for e in range(2):
            value = dot(picked[e], g[e, :, :, cols].reshape(groups * cap, width), 1, 0)
            weight_out[e, :, cols] = (value * slopes[e, :, cols].astype(F32)).astype(BF16)
            step_parts[p, pl.ds(e, 1), :] = jnp.sum(value * step_slopes[e, :, cols].astype(F32), axis=0, keepdims=True)
        @pl.when(n > 0)
        def _():
            grads(n).start()

        return carry

    own_steps.wait()
    for copy in steps_sent:
        copy.wait_recv()

    plan = (
        (2, x_second), (3, arrive(0)), (6, arrive(1)), (8, down(0)), (9, arrive(2)), (11, down(1)), (12, arrive(3)),
    )
    done = 0
    for until, event in plan:
        if until > done:
            lax.fori_loop(done, until, tile, 0)
            done = until
        event()
    lax.fori_loop(done, tiles, tile, 0)

    selections()
    far(0)()
    x_mid2()
    arrived(0)
    back(0)
    send_first(0)
    down(2)()
    far(1)()
    arrived(1)
    back(1)
    send_first(1)
    for ring in (x2a, x2b):
        ring.finish()
    down(3)()
    picks()
    far(2)()
    arrived(2)
    back(2)
    send_first(2)
    far(3)()
    arrived(3)
    back(3)
    send_first(3)
    second_a(1)
    lax.fori_loop(0, 1, raw, 0)
    s2a(1).start()
    lax.fori_loop(1, 4, raw, 0)
    second_a(2)
    lax.fori_loop(4, 5, raw, 0)
    s2a(2).start()
    lax.fori_loop(5, 7, raw, 0)
    second_a(3)
    lax.fori_loop(7, parts, raw, 0)
    s2a(3).start()
    second_b()
    lower = lower_sum(0)
    for k in range(1, 4):
        s2b(k).start()
    second_a(3, 1)
    upper = upper_sum(0)
    s2a(3, 1).start()
    s2a(3, 1).wait_recv()
    for r in range(1, 4):
        s2a(r).wait_recv()
        upper = upper + got_2a[r - 1].astype(F32)
    token_t[pl.ds(0, top)] = upper.astype(BF16)
    for k in range(1, 4):
        s2b(k).wait_recv()
        lower = lower + got_2b[k - 1].astype(F32)
    token_t[pl.ds(top, bottom)] = lower.astype(BF16)
    token_out[...] = token_t[...].T
    total = step_parts[part]
    for k in range(1, parts):
        grads(k).wait_recv()
        total = total + step_got[k - 1]
    step_out[...] = total * (qmax / math.sqrt(depth * parts * qmax))

    for copy in steps_sent + ids_sent:
        copy.wait_send()
    for r, k in pairs:
        a2a(r, k).wait_send()
    for ring in (x1a, x1b, x2a, x2b, *z_rings):
        ring.drain()
    for r in range(4):
        for n in range(4):
            to_pair(r, n).wait_send()
    for k in range(1, 4):
        for r in range(4):
            for c in range(2 if r == 3 else 1):
                s1a(r, k, c).wait_send()
        s1b(k).wait_send()
        s2a(k).wait_send()
        if k == 3:
            s2a(k, 1).wait_send()
        s2b(k).wait_send()
    for k in range(1, parts):
        grads(k).wait_send()


def layer(cot, tokens, ids, steps, weights):
    groups, parts = lax.axis_size("expert"), lax.axis_size("mp")
    e, d, f = weights.shape
    toks, width = tokens.shape
    cap, part_f = toks // 2, cot.shape[1]
    top = d * 5 // 7 // 16 * 16
    bottom = d - top
    dma = pltpu.SemaphoreType.DMA
    vmem = pl.BlockSpec(memory_space=pltpu.VMEM)
    anywhere = pl.BlockSpec(memory_space=pl.ANY)
    slots = e * cap

    def room(*shape, dtype=BF16):
        return pltpu.VMEM(shape, dtype)

    return pl.pallas_call(
        functools.partial(layer_kernel, cap),
        in_specs=[vmem] * 4 + [anywhere],
        out_specs=[vmem, vmem, vmem],
        out_shape=[
            pltpu.VMEM((toks, width), BF16),
            pltpu.VMEM((e, d, f), BF16),
            pltpu.VMEM((e, part_f), F32),
        ],
        scratch_shapes=[
            room(groups, e, cap, part_f),
            room(e, groups, cap, f),
            room(4, groups // 4, d, toks),
            room(groups, *ids.shape, dtype=jnp.int32),
            room(e, d, f), room(e, d, f), room(e, d, f),
            room(parts, *steps.shape, dtype=F32),
            room(2, TILE, f),
            room(groups // 2, 2 * slots, 2 * toks),
            room(e, d, groups * cap),
            room(e, d, 4 * cap),
            room(4, 4, d, toks),
            room(4, 3, top, toks),
            room(3, 4, bottom, toks),
            room(3, top, toks), room(3, bottom, toks), room(3, top, toks), room(3, bottom, toks),
            room(d, toks),
            room(parts, e, part_f, dtype=F32),
            room(parts - 1, e, part_f, dtype=F32),
            *[dma((4, 4))] * 8,
            *[dma((5, 4))] * 2, *[dma((4,))] * 6,
            dma((groups,)), dma((groups,)), dma((parts,)), dma((parts,)), dma((parts,)), dma((parts,)),
            dma((4,)), dma((2,)),
        ],
        compiler_params=pltpu.CompilerParams(collective_id=0, has_side_effects=True, vmem_limit_bytes=VMEM_LIMIT),
        name="layer",
    )(cot, tokens, ids, steps, weights)


def per_device(tokens, cotangent, weights, steps, expert_ids):
    toks, top_k = expert_ids.shape
    cot = cotangent.reshape(toks * top_k, cotangent.shape[2])
    return tuple(layer(cot, tokens, expert_ids.T, steps, weights))


def solution(mesh):
    return jax.shard_map(
        per_device,
        mesh=mesh,
        in_specs=(
            P("expert", "mp"),
            P("expert", None, "mp"),
            P("expert", "mp", None),
            P("expert", "mp"),
            P("expert", None),
        ),
        out_specs=(P("expert", "mp"), P("expert", "mp", None), P("expert", "mp")),
        check_vma=False,
    )
```

```python
import functools
import math

import jax
import jax.numpy as jnp
from jax import lax
from jax.experimental import pallas as pl
from jax.experimental.pallas import tpu as pltpu
from jax.sharding import PartitionSpec as P

qmax = 7.0
wiggle = 0.9
two_pi = 6.283185307179586
F32 = jnp.float32
BF16 = jnp.bfloat16

ROOT = math.sqrt(2.0 * wiggle)
SIN = tuple(ROOT * c for c in (3.141592640130707, -5.167710083507862, 2.550077523214134, -0.5982912856178576, 0.0776576603009221))
COS = tuple(
    2.0 * wiggle / (two_pi * qmax * ROOT) * c
    for c in (0.9999999532476082, -4.93479283061961, 4.058411352862034, -1.3318765680776314, 0.2196896110917421)
)


def poly(z, coefs):
    total = coefs[-1] * z + coefs[-2]
    for coef in coefs[-3::-1]:
        total = total * z + coef
    return total


def quantize(w, step7, inv7):
    t = w * inv7
    u = jnp.tanh(t)
    c = qmax * u
    r = c - jnp.round(c)
    z = r * r
    sine = r * poly(z, SIN)
    stair = u - sine * poly(z, COS)
    slopes = ((1.0 - wiggle) + sine * sine) * (1.0 - u * u)
    return step7 * stair, slopes, stair - t * slopes


def dot(a, b, ca, cb):
    return lax.dot_general(a, b, (((ca,), (cb,)), ((), ())), preferred_element_type=F32)


def upper(n):
    rows = lax.broadcasted_iota(jnp.int32, (n, n), 0)
    cols = lax.broadcasted_iota(jnp.int32, (n, n), 1)
    return jnp.where(rows < cols, 1.0, 0.0).astype(BF16)


def slots_of(ids_ref, cap, experts):
    choices, toks = ids_ref.shape
    routes = choices * toks
    expert = lax.broadcasted_iota(jnp.int32, (experts, toks), 0)
    hot = [jnp.where(expert == ids_ref[k : k + 1, :], 1.0, 0.0) for k in range(choices)]
    place = dot(functools.reduce(jnp.add, hot).astype(BF16), upper(toks), 1, 0)
    places = [jnp.sum(one * place, axis=0, keepdims=True) for one in hot]
    both = jnp.concatenate([ids_ref[...].astype(F32), *places], axis=0).astype(BF16)
    token = lax.broadcasted_iota(jnp.int32, (toks, routes), 0)
    route = lax.broadcasted_iota(jnp.int32, (toks, routes), 1)
    spread = dot(both, jnp.where(route // choices == token, 1.0, 0.0).astype(BF16), 1, 0)
    slots = spread[:choices] * float(cap) + spread[choices:]
    choice = lax.broadcasted_iota(jnp.int32, (choices, routes), 0)
    mine = lax.rem(lax.broadcasted_iota(jnp.int32, (choices, routes), 1), choices) == choice
    return jnp.sum(jnp.where(mine, slots, 0.0), axis=0, keepdims=True).astype(jnp.int32)


def selection(ids_ref, first, local, cap):
    groups, _, toks = ids_ref.shape
    ahead = upper(toks)
    picks = []
    for e in range(local):
        named = [jnp.max(jnp.where(ids_ref[i] == first + e, 1.0, 0.0), axis=0, keepdims=True) for i in range(groups)]
        named = jnp.concatenate(named, axis=0)
        place = dot(named.astype(BF16), ahead, 1, 0)
        picks.append(jnp.where(named > 0.0, place, -1.0).astype(jnp.int32))
    return picks


TILE = 128
VMEM_LIMIT = 52 << 20
STEP_COLS = 512
STEP_ROWS = 16


def ring4(pos, device, view, send, recv):
    up, down, far = lax.rem(pos + 1, 4), lax.rem(pos + 3, 4), lax.rem(pos + 2, 4)

    def copy(src, k, part, k_to, n):
        return pltpu.make_async_remote_copy(
            src_ref=view(k, part) if src is None else src,
            dst_ref=view(k, part),
            send_sem=send.at[n],
            recv_sem=recv.at[n],
            device_id=device(k_to),
            device_id_type=pl.DeviceIdType.MESH,
        )

    class Ring:
        def start(self, src=None):
            copy(src, pos, "all", up, 0).start()
            copy(src, pos, "all", down, 1).start()

        def from_down(self):
            copy(None, down, "all", up, 0).wait_recv()
            copy(None, down, "lo", up, 2).start()

        def from_up(self):
            copy(None, up, "all", down, 1).wait_recv()
            copy(None, up, "hi", down, 3).start()

        def finish(self):
            copy(None, far, "lo", up, 2).wait_recv()
            copy(None, far, "hi", down, 3).wait_recv()

        def drain(self):
            copy(None, pos, "all", up, 0).wait_send()
            copy(None, pos, "all", down, 1).wait_send()
            copy(None, down, "lo", up, 2).wait_send()
            copy(None, up, "hi", down, 3).wait_send()

    return Ring()


def all4(pos, device, view, send, recv):
    def copy(k, owner):
        return pltpu.make_async_remote_copy(
            src_ref=view(owner),
            dst_ref=view(owner),
            send_sem=send.at[k],
            recv_sem=recv.at[k],
            device_id=device(lax.rem(pos + k, 4)),
            device_id_type=pl.DeviceIdType.MESH,
        )

    class Direct:
        def start(self):
            for k in (1, 3, 2):
                copy(k, pos).start()

        def finish(self):
            for k in range(1, 4):
                copy(k, lax.rem(pos - k + 4, 4)).wait_recv()

        def drain(self):
            for k in range(1, 4):
                copy(k, pos).wait_send()

    return Direct()


def layer_kernel(
    cap, cot, tokens, ids, steps, weights,
    token_out, weight_out, step_out,
    packed, g, x, ids_all, q, slopes, step_slopes, steps_all, w_buf,
    select, picked, backs, partial, got_1a, got_1b, got_2a, got_2b, sum_a, sum_b, token_t, step_parts, step_got,
    a2a_send, a2a_recv, pair_send, pair_recv, z_send, z_recv, x_send, x_recv,
    s1a_send, s1a_recv, s1b_send, s1b_recv, s2a_send, s2a_recv, s2b_send, s2b_recv,
    ids_send, ids_recv, steps_send, steps_recv, grads_send, grads_recv, own_sem, w_sem,
):
    me, part = lax.axis_index("expert"), lax.axis_index("mp")
    groups, parts = lax.axis_size("expert"), lax.axis_size("mp")
    row, col = me // 4, lax.rem(me, 4)
    z, core = part // 2, lax.rem(part, 2)
    width = cot.shape[-1]
    depth = tokens.shape[1]

    def remote(src, dst, send, recv, expert, mp):
        return pltpu.make_async_remote_copy(
            src_ref=src, dst_ref=dst, send_sem=send, recv_sem=recv,
            device_id=(expert, mp), device_id_type=pl.DeviceIdType.MESH,
        )

    barrier = pltpu.get_barrier_semaphore()
    for k in range(1, groups):
        pl.semaphore_signal(barrier, 1, device_id=(lax.rem(me + k, groups), part), device_id_type=pl.DeviceIdType.MESH)
    for k in range(1, parts):
        pl.semaphore_signal(barrier, 1, device_id=(me, lax.rem(part + k, parts)), device_id_type=pl.DeviceIdType.MESH)
    first_w = pltpu.make_async_copy(weights.at[0, pl.ds(0, TILE), :], w_buf.at[0], w_sem.at[0])
    first_w.start()

    def lanes(p):
        return pl.ds(pl.multiple_of(p * width, width), width)

    own_g = pltpu.make_async_copy(packed.at[me], g.at[:, me, :, lanes(part)], own_sem.at[0])
    own_ids = pltpu.make_async_copy(ids, ids_all.at[me], own_sem.at[2])
    own_steps = pltpu.make_async_copy(steps, steps_all.at[part], own_sem.at[3])
    for own in (own_ids, own_steps):
        own.start()

    x[row, col] = tokens[...].T
    slot_row = slots_of(ids, cap, groups * 2)
    slot = lax.broadcasted_iota(jnp.int32, (2 * cap, slot_row.shape[1]), 0)

    def pack(n, carry):
        to = lax.rem(row - n // 4 + 4, 4) * 4 + lax.rem(col + n, 4)
        pick = jnp.where(slot == slot_row - to * (2 * cap), 1.0, 0.0).astype(BF16)
        packed[to] = dot(pick, cot[...], 1, 0).astype(BF16).reshape(2, cap, width)
        return carry

    pl.semaphore_wait(barrier, groups + parts - 2)

    steps_sent = [
        remote(steps, steps_all.at[part], steps_send.at[k], steps_recv.at[k], me, lax.rem(part + k, parts))
        for k in range(1, parts)
    ]
    for copy in steps_sent:
        copy.start()

    def a2a(r, k):
        to = lax.rem(row - r + 4, 4) * 4 + lax.rem(col + k, 4)
        return remote(packed.at[to], g.at[:, me, :, lanes(part)], a2a_send.at[r, k], a2a_recv.at[r, k], to, part)

    def a2a_wait(r):
        for k in range(4):
            if r or k:
                source = lax.rem(row + r, 4) * 4 + lax.rem(col - k + 4, 4)
                remote(packed.at[source], g.at[:, source, :, lanes(part)], a2a_send.at[r, k], a2a_recv.at[r, k], source, part).wait_recv()

    half = depth // 2

    def on_x(k):
        return (row * 4 + k, part)

    def on_y(k):
        return (k * 4 + col, part)

    def x_pair(piece):
        return pl.ds(2 if piece == "hi" else 0, 4 if piece == "all" else 2)

    x1a = all4(col, on_x, lambda k: x.at[row, k, pl.ds(0, half)], x_send.at[0], x_recv.at[0])
    x1b = all4(row, on_y, lambda k: x.at[k, col, pl.ds(half, half)], x_send.at[1], x_recv.at[1])
    x2a = ring4(row, on_y, lambda k, piece: x.at[k, x_pair(piece), pl.ds(0, half)], x_send.at[2], x_recv.at[2])
    x2b = ring4(col, on_x, lambda k, piece: x.at[x_pair(piece), k, pl.ds(half, half)], x_send.at[3], x_recv.at[3])
    x1a.start()
    x1b.start()
    lax.fori_loop(0, groups // 2, pack, 0)
    own_g.start()
    pairs = [(r, k) for r in range(4) for k in range(4) if r or k]
    for r, k in pairs[:7]:
        a2a(r, k).start()
    ids_sent = [
        remote(ids, ids_all.at[me], ids_send.at[k], ids_recv.at[k], lax.rem(me + k, groups), part) for k in range(1, groups)
    ]
    for copy in ids_sent:
        copy.start()
    lax.fori_loop(groups // 2, groups, pack, 0)
    for r, k in pairs[7:]:
        a2a(r, k).start()

    def on_z(k):
        return (me, k * 2 + core)

    def g_view(r, owner):
        sources = pl.ds(pl.multiple_of(lax.rem(row + r, 4) * 4, 4), 4)

        def view(k, piece):
            some = {"all": pl.ds(0, 2), "lo": pl.ds(0, 1), "hi": pl.ds(1, 1)}[piece]
            return g.at[some, sources, :, lanes(k * 2 + owner)]

        return view

    z_rings = [ring4(z, on_z, g_view(r, core), z_send.at[r], z_recv.at[r]) for r in range(4)]

    def to_pair(r, n):
        view = g_view(r, core)(lax.rem(z + (0, 3, 1, 2)[n], 4), "all")
        return remote(view, view, pair_send.at[r, n], pair_recv.at[r, n], me, z * 2 + 1 - core)

    def from_pair(r, n):
        view = g_view(r, 1 - core)(lax.rem(z + (0, 3, 1, 2)[n], 4), "all")
        return remote(view, view, pair_send.at[r, n], pair_recv.at[r, n], me, z * 2 + 1 - core)

    def arrive(r):
        def event():
            a2a_wait(r)
            if r == 0:
                own_g.wait()
            z_rings[r].start()
            to_pair(r, 0).start()

        return event

    def down(r):
        def event():
            z_rings[r].from_down()
            to_pair(r, 1).start()
            z_rings[r].from_up()
            to_pair(r, 2).start()

        return event

    def far(r):
        def event():
            z_rings[r].finish()
            to_pair(r, 3).start()

        return event

    def x_second():
        for ring, other in ((x1a, x2a), (x1b, x2b)):
            ring.finish()
            other.start()

    def x_mid2():
        for ring in (x2a, x2b):
            ring.from_down()
            ring.from_up()

    tiles_each = weights.shape[1] // TILE
    tiles = weights.shape[0] * tiles_each

    def w_in(t, slot):
        at = pl.ds(pl.multiple_of(lax.rem(t, tiles_each) * TILE, TILE), TILE)
        return pltpu.make_async_copy(weights.at[t // tiles_each, at, :], w_buf.at[slot], w_sem.at[slot])

    def tile(t, carry):
        slot = lax.rem(t, 2)
        w_in(t, slot).wait()

        @pl.when(t + 1 < tiles)
        def _():
            w_in(t + 1, 1 - slot).start()

        e = t // tiles_each
        head = lax.rem(t, tiles_each) * TILE

        def chunk(j, carry):
            cols = pl.ds(pl.multiple_of(j * STEP_COLS, STEP_COLS), STEP_COLS)
            per = STEP_COLS // width
            s = jnp.concatenate([steps_all[j * per + n, pl.ds(e, 1), :] for n in range(per)], axis=1)
            step7 = qmax * s
            inv7 = 1.0 / step7

            def rows(k, carry):
                at = pl.ds(pl.multiple_of(k * STEP_ROWS, STEP_ROWS), STEP_ROWS)
                to = pl.ds(pl.multiple_of(head + k * STEP_ROWS, STEP_ROWS), STEP_ROWS)
                level, slope, step_slope = quantize(w_buf[slot, at, cols].astype(F32), step7, inv7)
                q[e, to, cols] = level.astype(BF16)
                slopes[e, to, cols] = slope.astype(BF16)
                step_slopes[e, to, cols] = step_slope.astype(BF16)
                return carry

            return lax.fori_loop(0, TILE // STEP_ROWS, rows, carry, unroll=2)

        lax.fori_loop(0, weights.shape[2] // STEP_COLS, chunk, 0)
        return carry

    top = sum_a.shape[1]
    bottom = depth - top

    def block_rows(r):
        return pl.multiple_of(lax.rem(row + r, 4) * 4, 4)

    def arrived(r):
        for n in range(4):
            from_pair(r, n).wait_recv()

    def selections():
        own_ids.wait()
        for copy in ids_sent:
            copy.wait_recv()
        places = selection(ids_all, me * 2, 2, cap)
        slot = lax.broadcasted_iota(jnp.int32, (2 * cap, 2 * ids.shape[1]), 0)
        for e in range(2):
            for n in range(groups // 2):
                first, second = places[e][2 * n : 2 * n + 1], places[e][2 * n + 1 : 2 * n + 2]
                place = jnp.concatenate([first, jnp.where(second < 0, second, second + cap)], axis=1)
                select[n, pl.ds(e * 2 * cap, 2 * cap)] = jnp.where(slot == place, 1.0, 0.0).astype(BF16)

    def picks():
        def one(n, carry):
            both = jnp.concatenate([x[n // 2, 2 * lax.rem(n, 2)], x[n // 2, 2 * lax.rem(n, 2) + 1]], axis=1)
            out = dot(both, select[n], 1, 1).astype(BF16)
            at = pl.ds(pl.multiple_of(n * 2 * cap, 2 * cap), 2 * cap)
            for e in range(2):
                picked[e, :, at] = out[:, 2 * cap * e : 2 * cap * (e + 1)]
            return carry

        lax.fori_loop(0, groups // 2, one, 0)

    def back(r):
        base = block_rows(r)
        for e in range(2):
            backs[e] = dot(q[e], g[e, pl.ds(base, 4)].reshape(4 * cap, -1), 1, 1).astype(BF16)
        for n in range(2):
            both = jnp.concatenate([backs[e, :, 2 * cap * n : 2 * cap * (n + 1)] for e in range(2)], axis=1)
            out = dot(both, select[base // 2 + n], 1, 0).astype(BF16)
            for k in range(2):
                partial[r, 2 * n + k] = out[:, 2 * cap * k : 2 * cap * (k + 1)]

    cut = top // 32 * 16

    def piece(r, c):
        if r < 3:
            return pl.ds(0, top)
        return pl.ds(cut, top - cut) if c else pl.ds(0, cut)

    def s1a(r, k, c=0):
        to = lax.rem(col + k, 4)
        return remote(
            partial.at[r, to, piece(r, c)], got_1a.at[r, k - 1, piece(r, c)], s1a_send.at[r + c, k], s1a_recv.at[r + c, k],
            row * 4 + to, part,
        )

    def s1b(r):
        to = lax.rem(row + r, 4)
        return remote(
            partial.at[r, :, pl.ds(top, bottom)], got_1b.at[r - 1], s1b_send.at[r], s1b_recv.at[r], to * 4 + col, part
        )

    def s2a(r, c=0):
        to = lax.rem(row + r, 4)
        n = 0 if c else r
        return remote(
            sum_a.at[r - 1, piece(r, c)], got_2a.at[r - 1, piece(r, c)], s2a_send.at[n], s2a_recv.at[n], to * 4 + col, part
        )

    def s2b(k):
        to = lax.rem(col + k, 4)
        return remote(sum_b.at[k - 1], got_2b.at[k - 1], s2b_send.at[k], s2b_recv.at[k], row * 4 + to, part)

    def send_first(r):
        for c in range(2 if r == 3 else 1):
            for k in (1, 3, 2):
                s1a(r, k, c).start()
        if r:
            s1b(r).start()

    def upper_sum(r, c=0):
        for k in range(1, 4):
            s1a(r, k, c).wait_recv()
        total = partial[r, col, piece(r, c)].astype(F32)
        for k in range(3):
            total = total + got_1a[r, k, piece(r, c)].astype(F32)
        return total

    def second_a(r, c=0):
        sum_a[r - 1, piece(r, c)] = upper_sum(r, c).astype(BF16)

    def lower_sum(k):
        to = lax.rem(col + k, 4)
        total = partial[0, to, pl.ds(top, bottom)].astype(F32)
        for r in range(3):
            total = total + got_1b[r, to].astype(F32)
        return total

    def second_b():
        for r in range(1, 4):
            s1b(r).wait_recv()
        for k in range(1, 4):
            sum_b[k - 1] = lower_sum(k).astype(BF16)

    def grads(k):
        to = lax.rem(part + k, parts)
        return remote(step_parts.at[to], step_got.at[k - 1], grads_send.at[k], grads_recv.at[k], me, to)

    def raw(n, carry):
        p = lax.rem(part + 1 + n, parts)
        cols = lanes(p)

        for e in range(2):
            value = dot(picked[e], g[e, :, :, cols].reshape(groups * cap, width), 1, 0)
            weight_out[e, :, cols] = (value * slopes[e, :, cols].astype(F32)).astype(BF16)
            step_parts[p, pl.ds(e, 1), :] = jnp.sum(value * step_slopes[e, :, cols].astype(F32), axis=0, keepdims=True)
        @pl.when(n > 0)
        def _():
            grads(n).start()

        return carry

    own_steps.wait()
    for copy in steps_sent:
        copy.wait_recv()

    plan = (
        (2, x_second), (3, arrive(0)), (6, arrive(1)), (8, down(0)), (9, arrive(2)), (11, down(1)), (12, arrive(3)),
    )
    done = 0
    for until, event in plan:
        if until > done:
            lax.fori_loop(done, until, tile, 0)
            done = until
        event()
    lax.fori_loop(done, tiles, tile, 0)

    selections()
    far(0)()
    x_mid2()
    arrived(0)
    back(0)
    send_first(0)
    down(2)()
    far(1)()
    arrived(1)
    back(1)
    send_first(1)
    for ring in (x2a, x2b):
        ring.finish()
    down(3)()
    picks()
    far(2)()
    arrived(2)
    back(2)
    send_first(2)
    far(3)()
    arrived(3)
    back(3)
    send_first(3)
    second_a(1)
    lax.fori_loop(0, 1, raw, 0)
    s2a(1).start()
    lax.fori_loop(1, 4, raw, 0)
    second_a(2)
    lax.fori_loop(4, 5, raw, 0)
    s2a(2).start()
    lax.fori_loop(5, 7, raw, 0)
    second_a(3)
    lax.fori_loop(7, parts, raw, 0)
    s2a(3).start()
    second_b()
    lower = lower_sum(0)
    for k in range(1, 4):
        s2b(k).start()
    second_a(3, 1)
    upper = upper_sum(0)
    s2a(3, 1).start()
    s2a(3, 1).wait_recv()
    for r in range(1, 4):
        s2a(r).wait_recv()
        upper = upper + got_2a[r - 1].astype(F32)
    token_t[pl.ds(0, top)] = upper.astype(BF16)
    for k in range(1, 4):
        s2b(k).wait_recv()
        lower = lower + got_2b[k - 1].astype(F32)
    token_t[pl.ds(top, bottom)] = lower.astype(BF16)
    token_out[...] = token_t[...].T
    total = step_parts[part]
    for k in range(1, parts):
        grads(k).wait_recv()
        total = total + step_got[k - 1]
    step_out[...] = total * (qmax / math.sqrt(depth * parts * qmax))

    for copy in steps_sent + ids_sent:
        copy.wait_send()
    for r, k in pairs:
        a2a(r, k).wait_send()
    for ring in (x1a, x1b, x2a, x2b, *z_rings):
        ring.drain()
    for r in range(4):
        for n in range(4):
            to_pair(r, n).wait_send()
    for k in range(1, 4):
        for r in range(4):
            for c in range(2 if r == 3 else 1):
                s1a(r, k, c).wait_send()
        s1b(k).wait_send()
        s2a(k).wait_send()
        if k == 3:
            s2a(k, 1).wait_send()
        s2b(k).wait_send()
    for k in range(1, parts):
        grads(k).wait_send()


def layer(cot, tokens, ids, steps, weights):
    groups, parts = lax.axis_size("expert"), lax.axis_size("mp")
    e, d, f = weights.shape
    toks, width = tokens.shape
    cap, part_f = toks // 2, cot.shape[1]
    top = d * 5 // 7 // 16 * 16
    bottom = d - top
    dma = pltpu.SemaphoreType.DMA
    vmem = pl.BlockSpec(memory_space=pltpu.VMEM)
    anywhere = pl.BlockSpec(memory_space=pl.ANY)
    slots = e * cap

    def room(*shape, dtype=BF16):
        return pltpu.VMEM(shape, dtype)

    return pl.pallas_call(
        functools.partial(layer_kernel, cap),
        in_specs=[vmem] * 4 + [anywhere],
        out_specs=[vmem, vmem, vmem],
        out_shape=[
            pltpu.VMEM((toks, width), BF16),
            pltpu.VMEM((e, d, f), BF16),
            pltpu.VMEM((e, part_f), F32),
        ],
        scratch_shapes=[
            room(groups, e, cap, part_f),
            room(e, groups, cap, f),
            room(4, groups // 4, d, toks),
            room(groups, *ids.shape, dtype=jnp.int32),
            room(e, d, f), room(e, d, f), room(e, d, f),
            room(parts, *steps.shape, dtype=F32),
            room(2, TILE, f),
            room(groups // 2, 2 * slots, 2 * toks),
            room(e, d, groups * cap),
            room(e, d, 4 * cap),
            room(4, 4, d, toks),
            room(4, 3, top, toks),
            room(3, 4, bottom, toks),
            room(3, top, toks), room(3, bottom, toks), room(3, top, toks), room(3, bottom, toks),
            room(d, toks),
            room(parts, e, part_f, dtype=F32),
            room(parts - 1, e, part_f, dtype=F32),
            *[dma((4, 4))] * 8,
            *[dma((5, 4))] * 2, *[dma((4,))] * 6,
            dma((groups,)), dma((groups,)), dma((parts,)), dma((parts,)), dma((parts,)), dma((parts,)),
            dma((4,)), dma((2,)),
        ],
        compiler_params=pltpu.CompilerParams(collective_id=0, has_side_effects=True, vmem_limit_bytes=VMEM_LIMIT),
        name="layer",
    )(cot, tokens, ids, steps, weights)


def per_device(tokens, cotangent, weights, steps, expert_ids):
    toks, top_k = expert_ids.shape
    cot = cotangent.reshape(toks * top_k, cotangent.shape[2])
    return tuple(layer(cot, tokens, expert_ids.T, steps, weights))


def solution(mesh):
    return jax.shard_map(
        per_device,
        mesh=mesh,
        in_specs=(
            P("expert", "mp"),
            P("expert", None, "mp"),
            P("expert", "mp", None),
            P("expert", "mp"),
            P("expert", None),
        ),
        out_specs=(P("expert", "mp"), P("expert", "mp", None), P("expert", "mp")),
        check_vma=False,
    )
```
